32 devices in a mesh: dp: 4 (over x, y), tp: 8 (over z, core).
Axes of the slice: x: 2, y: 2, z: 4, core: 2. Of those that a mesh axis runs over, the one named last changes fastest.
Arguments:
- x: bfloat16 [16, 512, 5120], P('dp'), parts along dimension 0
- gain_a: bfloat16 [5120], replicated
- wq: bfloat16 [5120, 8192], P(None, 'tp')
- wk: bfloat16 [5120, 1024], P(None, 'tp')
- wv: bfloat16 [5120, 1024], P(None, 'tp')
- wo: bfloat16 [8192, 5120], P('tp')
- gain_m: bfloat16 [5120], replicated
- w_gate: bfloat16 [5120, 25600], P(None, 'tp')
- w_up: bfloat16 [5120, 25600], P(None, 'tp')
- w_down: bfloat16 [25600, 5120], P('tp')
Outputs:
- output: bfloat16 [16, 512, 5120], P('dp'), parts along dimension 0
There are 4 independent parts. The reference program is written for one: setup_inputs(seed, part) draws one part's arguments, and reference() takes and returns one part's arrays. A program takes and returns all parts, laid end to end along the dimension named above; an argument that names none is the same for every part.
All inputs are finite; a program needn't handle non-finite values.
Results may differ from the reference program's by a relative error of at most 0.017.
Values are sent between devices in bfloat16 or wider.
A program may use at most 2 GiB of HBM per device.

```python
import jax
import jax.numpy as jnp
from jax import lax

SEQUENCES = 4
TOKENS = 512
D = 5120
HEADS = 64
KV_HEADS = 8
HEAD = 128
FF = 25600
THETA = 10000


def setup_inputs(seed: int = 0, part: int = 0) -> dict:
    kx, ka, km, kq, kk, kv, ko, kg, ku, kd = jax.random.split(jax.random.key(seed), 10)

    def weights(key, rows, columns):
        return jax.random.normal(key, (rows, columns), jnp.float32) * rows**-0.5

    drawn = {
        "x": jax.random.normal(jax.random.fold_in(kx, part), (SEQUENCES, TOKENS, D), jnp.float32),
        "gain_a": 1 + 0.1 * jax.random.normal(ka, (D,), jnp.float32),
        "wq": 2 * weights(kq, D, HEADS * HEAD),
        "wk": 2 * weights(kk, D, KV_HEADS * HEAD),
        "wv": 4 * weights(kv, D, KV_HEADS * HEAD),
        "wo": weights(ko, HEADS * HEAD, D),
        "gain_m": 1 + 0.1 * jax.random.normal(km, (D,), jnp.float32),
        "w_gate": weights(kg, D, FF),
        "w_up": weights(ku, D, FF),
        "w_down": 3 * weights(kd, FF, D),
    }
    return {k: v.astype(jnp.bfloat16) for k, v in drawn.items()}


def normed(x, gain):
    wide = x.astype(jnp.float32)
    scale = lax.rsqrt(jnp.mean(wide * wide, -1, keepdims=True) + 1e-6)
    return (wide * scale * gain.astype(jnp.float32)).astype(jnp.bfloat16)


def turned(t, place, theta):
    half = t.shape[-1] // 2
    angle = place.astype(jnp.float32)[:, None] * theta ** (-jnp.arange(half, dtype=jnp.float32) / half)
    cos, sin = jnp.cos(angle)[:, None], jnp.sin(angle)[:, None]
    a, b = t[..., :half].astype(jnp.float32), t[..., half:].astype(jnp.float32)
    return jnp.concatenate([a * cos - b * sin, b * cos + a * sin], -1).astype(jnp.bfloat16)


def matmul(a, w):
    return jnp.dot(a, w, preferred_element_type=jnp.float32).astype(jnp.bfloat16)


def einsum(form, a, b):
    return jnp.einsum(form, a.astype(jnp.float32), b.astype(jnp.float32))


def attention(q, k, v):
    scores = einsum("tgsd,ugd->gstu", q, k) * q.shape[-1] ** -0.5
    token = jnp.arange(q.shape[0])
    scores = jnp.where(token[:, None] >= token, scores, -jnp.inf)
    weights = jax.nn.softmax(scores, -1).astype(jnp.bfloat16)
    return einsum("gstu,ugd->tgsd", weights, v).astype(jnp.bfloat16)


def one(x, gain_a, wq, wk, wv, wo, gain_m, w_gate, w_up, w_down):
    rows = x.shape[0]
    a, place = normed(x, gain_a), jnp.arange(rows)
    k = turned(matmul(a, wk).reshape(rows, -1, HEAD), place, THETA)
    q = turned(matmul(a, wq).reshape(rows, -1, HEAD), place, THETA).reshape(rows, k.shape[1], -1, HEAD)
    v = matmul(a, wv).reshape(rows, -1, HEAD)
    seen = attention(q, k, v).reshape(rows, -1)
    h = (x.astype(jnp.float32) + jnp.dot(seen, wo, preferred_element_type=jnp.float32)).astype(jnp.bfloat16)
    b = normed(h, gain_m)
    gate = jnp.dot(b, w_gate, preferred_element_type=jnp.float32)
    up = jnp.dot(b, w_up, preferred_element_type=jnp.float32)
    hidden = (jax.nn.silu(gate) * up).astype(jnp.bfloat16)
    return (h.astype(jnp.float32) + jnp.dot(hidden, w_down, preferred_element_type=jnp.float32)).astype(jnp.bfloat16)


def reference(x, gain_a, wq, wk, wv, wo, gain_m, w_gate, w_up, w_down):
    return lax.map(lambda sequence: one(sequence, gain_a, wq, wk, wv, wo, gain_m, w_gate, w_up, w_down), x)
```

```python
import functools

import jax
import jax.numpy as jnp
from jax import lax
from jax.experimental import pallas as pl
from jax.experimental.pallas import tpu as pltpu
from jax.sharding import PartitionSpec as P

HEAD = 128
THETA = 10000
MESH = pl.DeviceIdType.MESH
LOG2E = 1.4426950408889634
HIDDEN = -2e30
COL = 256
UP = 8
PAIR = 4
DEPTH = 3
STRIP = 32


def both(a, b):
    return jnp.logical_and(a, b)


def mod(a, n):
    return lax.rem(a, n)


def div(a, n):
    return lax.div(a, n)


class Plan:
    def __init__(self, seqs, rows, d, kq, ff):
        self.seqs, self.rows, self.d, self.kq, self.ff = seqs, rows, d, kq, ff
        self.half = rows // 2
        self.heads = kq // HEAD
        self.nc = d // COL
        self.pieces = 2 * seqs * self.nc
        self.nq = kq // COL + 1
        self.per = d // kq
        self.nw = self.nc // self.per
        self.ng = ff // 128
        self.la, self.lm = self.nq + self.nw, self.ng + self.nc
        full = self.nc == 20
        self.before, self.inwo, self.offset, self.lead = (6, 6, 6, 18) if full else (1, 2, 1, 2)
        self.gu, self.dn = (17, 9) if full else (2, 2)
        self.slots = 44 if full else 14
        self.ka = self.before + self.inwo
        self.km = self.gu + self.dn
        self.a_end = self.ka * seqs - self.offset
        self.blocks = rows // 128
        self.lag = 7

    def a_pre(self, i, k, n):
        return self.ka * i - self.offset + div(self.before * (k + 1), n)

    def a_wo(self, i, j):
        return self.ka * i - self.offset + self.before + jnp.minimum(div(self.inwo * j + self.lead, self.nc), self.inwo)

    def m_gu(self, i, j):
        return self.a_end + self.km * i + div(self.gu * (j + 1), self.ng)

    def m_dn(self, i, j):
        last = self.a_end + self.km * i + self.gu + (j + 1)
        return jnp.where(i == self.seqs - 1, last, self.a_end + self.km * i + self.gu + div(self.dn * (j + 1), self.nc))


def kernel(pn, x_ref, ga_ref, gm_ref, rc_ref, rs_ref, wq_ref, wk_ref, wv_ref, wo_ref, wg_ref, wu_ref, wd_ref, y_ref,
           hbuf, abuf, wbuf, hid, q_s, k_s, v_s, own, dsend, drecv, usend, zrecv, mrecv, acc_s,
           x_sem, w_sem, y_sem, d_ss, d_rs, u_ss, z_rs, m_rs, f_ss, f_rs, g_ss, g_rs):
    f32, low = jnp.float32, jnp.bfloat16
    T, H, NC, NP, HALF = pn.rows, pn.half, pn.nc, pn.pieces, pn.pieces // 2
    t_me = lax.axis_index("tp")
    z, c = div(t_me, 2), mod(t_me, 2)
    is_end = mod(z, 3) == 0
    is_mid = mod(z, 3) != 0
    partner = z * 2 + 1 - c
    pair = (z + 1 - 2 * mod(z, 2)) * 2 + c
    across = (3 - z) * 2 + c

    def remote(src, dst, ss, rs, to):
        return pltpu.make_async_remote_copy(src_ref=src, dst_ref=dst, send_sem=ss, recv_sem=rs, device_id={"tp": to}, device_id_type=MESH)

    def d_copy(s):
        return remote(dsend.at[s], drecv.at[s], d_ss.at[s], d_rs.at[s], partner)

    def z_copy(s):
        return remote(usend.at[s], zrecv.at[s], u_ss.at[s], z_rs.at[s], pair)

    def m_copy(s):
        return remote(usend.at[s], mrecv.at[s], u_ss.at[s], m_rs.at[s], across)

    def place(p):
        q = mod(p, HALF)
        return mod(q, NC), pl.multiple_of(div(q, NC) * T, T)

    def mine(p):
        j, row = place(p)
        return hbuf.at[j, pl.ds(pl.multiple_of(row + c * H, H), H), :]

    def f_copy(p):
        s = mod(p, UP)
        return remote(mine(p), mine(p), f_ss.at[s], f_rs.at[s], pair)

    def g_copy(p):
        s = mod(p, UP)
        return remote(mine(p), mine(p), g_ss.at[s], g_rs.at[s], partner)

    def y_copy(p):
        j, row = place(p)
        return pltpu.make_async_copy(hbuf.at[j, pl.ds(row, T), :],
                                     y_ref.at[pl.ds(row, T), pl.ds(pl.multiple_of(j * COL, COL), COL)], y_sem.at[mod(p, UP)])

    def tick(t):
        @pl.when(both(is_end, t < NP))
        def _():
            s = mod(t, UP)

            @pl.when(t >= UP)
            def _():
                z_copy(s).wait_send()

            usend[s] = own[mod(t, pn.slots)].astype(low)
            z_copy(s).start()

        pm = t - 2

        @pl.when(both(is_mid, both(pm >= 0, pm < NP)))
        def _():
            s = mod(pm, UP)
            z_copy(s).wait_recv()

            @pl.when(pm >= UP)
            def _():
                m_copy(s).wait_send()

            usend[s] = (own[mod(pm, pn.slots)] + zrecv[s].astype(f32)).astype(low)
            m_copy(s).start()

        pf = t - 4

        @pl.when(both(is_mid, both(pf >= 0, pf < NP)))
        def _():
            s = mod(pf, UP)
            m_copy(s).wait_recv()

            @pl.when(pf >= UP)
            def _():
                f_copy(pf).wait_send()
                g_copy(pf).wait_send()

            at = mine(pf)
            at[...] = (at[...].astype(f32) + (usend[s].astype(f32) + mrecv[s].astype(f32))).astype(low)
            f_copy(pf).start()
            g_copy(pf).start()

        pe = t - 6

        @pl.when(both(is_end, both(pe >= 0, pe < NP)))
        def _():
            f_copy(pe).wait_recv()

            @pl.when(pe >= UP)
            def _():
                g_copy(pe).wait_send()

            g_copy(pe).start()

        pg = t - pn.lag

        @pl.when(both(pg >= 0, pg < NP))
        def _():
            g_copy(pg).wait_recv()

            @pl.when(pg >= HALF)
            def _():
                @pl.when(pg >= HALF + UP)
                def _():
                    y_copy(pg).wait()

                y_copy(pg).start()

    def ticks(lo, hi):
        def one(t, carry):
            tick(t)
            return carry

        lax.fori_loop(jnp.maximum(lo, 0), jnp.maximum(hi, 0), one, 0)

    def combine(p):
        s = mod(p, PAIR)
        d_copy(s).wait_recv()
        o = mod(p, pn.slots)
        own[o] = own[o] + drecv[s].astype(f32)

    def produce(acc, p, first):
        s = mod(p, PAIR)

        @pl.when(p >= PAIR)
        def _():
            d_copy(s).wait_send()

        dsend[s] = acc[H:, :].astype(low)
        own[mod(p, pn.slots)] = acc[:H, :]
        d_copy(s).start()

        @pl.when(jnp.logical_not(first))
        def _():
            combine(p - 1)

    def cols(ref, j, n):
        return ref.at[:, pl.ds(pl.multiple_of(j * n, n), n)]

    def load_q(l, s):
        return [pltpu.make_async_copy(cols(wq_ref, l, COL), wbuf.at[s], w_sem.at[s, 0])]

    def load_kv(s):
        return [pltpu.make_async_copy(wk_ref, wbuf.at[s, :, pl.ds(0, HEAD)], w_sem.at[s, 0]),
                pltpu.make_async_copy(wv_ref, wbuf.at[s, :, pl.ds(HEAD, HEAD)], w_sem.at[s, 1])]

    def load_o(l, s):
        return [pltpu.make_async_copy(cols(wo_ref, l * pn.per + k, COL), wbuf.at[s, pl.ds(k * pn.kq, pn.kq), :], w_sem.at[s, k])
                for k in range(pn.per)]

    def load_gu(l, s):
        return [pltpu.make_async_copy(cols(wg_ref, l, 128), wbuf.at[s, :, pl.ds(0, 128)], w_sem.at[s, 0]),
                pltpu.make_async_copy(cols(wu_ref, l, 128), wbuf.at[s, :, pl.ds(128, 128)], w_sem.at[s, 1])]

    def load_d(l, s):
        return [pltpu.make_async_copy(cols(wd_ref, l, COL), wbuf.at[s, pl.ds(0, pn.ff), :], w_sem.at[s, 0])]

    def start(copies):
        for x in copies:
            x.start()

    def wait(copies):
        for x in copies:
            x.wait()

    def start_a(l):
        s = mod(l, DEPTH)

        @pl.when(l < pn.nq - 1)
        def _():
            start(load_q(l, s))

        @pl.when(l == pn.nq - 1)
        def _():
            start(load_kv(s))

        @pl.when(l >= pn.nq)
        def _():
            start(load_o(l - pn.nq, s))

    def start_m(l):
        s = mod(l, DEPTH)

        @pl.when(l < pn.ng)
        def _():
            start(load_gu(l, s))

        @pl.when(l >= pn.ng)
        def _():
            start(load_d(l - pn.ng, s))

    def ahead_a(i, l):
        n = l + DEPTH - 1

        @pl.when(n < pn.la)
        def _():
            start_a(n)

        @pl.when(both(n >= pn.la, i < pn.seqs - 1))
        def _():
            start_a(n - pn.la)

        @pl.when(both(n >= pn.la, i == pn.seqs - 1))
        def _():
            start_m(n - pn.la)

    def ahead_m(i, l):
        n = l + DEPTH - 1

        @pl.when(n < pn.lm)
        def _():
            start_m(n)

        @pl.when(both(n >= pn.lm, i < pn.seqs - 1))
        def _():
            start_m(n - pn.lm)

    def norm(i, g_ref, shift):
        def strip(s, carry):
            rows = pl.ds(pl.multiple_of(i * T + s * STRIP, STRIP), STRIP)
            total = jnp.zeros((STRIP, COL), f32)
            for j in range(NC):
                v = hbuf[j, rows, :].astype(f32)
                total += v * v
            scale = lax.rsqrt(jnp.sum(total, axis=-1, keepdims=True) * (1.0 / pn.d) + 1e-6)
            to = pl.ds(pl.multiple_of(mod(s * STRIP + shift, T), STRIP), STRIP)
            for j in range(NC):
                v = hbuf[j, rows, :].astype(f32)
                abuf[to, j * COL : (j + 1) * COL] = (v * scale * g_ref[:, j * COL : (j + 1) * COL].astype(f32)).astype(low)
            return carry

        lax.fori_loop(0, T // STRIP, strip, 0)

    def turn(t):
        t = t.astype(low).astype(f32)
        return (t * rc_ref[...] + pltpu.roll(t, HEAD // 2, 1) * rs_ref[...]).astype(low)

    def attention(i):
        e = HEAD**-0.5 * LOG2E
        wide = pn.heads * 128
        gap = mod(lax.broadcasted_iota(jnp.int32, (128, wide), 1), 128) - lax.broadcasted_iota(jnp.int32, (128, wide), 0)
        for b in range(pn.blocks):
            nk = (b + 1) * 128
            q = q_s[:, b * 128 : (b + 1) * 128, :].reshape(wide, HEAD)
            s = lax.dot_general(k_s[:nk, :], q, (((1,), (1,)), ((), ())), preferred_element_type=f32)
            last = jnp.where(gap >= 0, s[b * 128 :, :], HIDDEN)
            s = last if b == 0 else jnp.concatenate([s[: b * 128, :], last], axis=0)
            p = jnp.exp2((s - s.max(axis=0, keepdims=True)) * e).astype(low)
            values = jnp.concatenate([v_s[:nk, :].T, jnp.ones((8, nk), low)], axis=0)
            o = lax.dot_general(values, p, (((1,), (0,)), ((), ())), preferred_element_type=f32)
            o = (o[:HEAD, :] * (1.0 / o[HEAD : HEAD + 1, :])).T.astype(low)
            to = pl.ds(pl.multiple_of(mod(b * 128 + c * H, T), 128), 128)
            for n in range(pn.heads):
                hid[to, n * HEAD : (n + 1) * HEAD] = o[n * 128 : (n + 1) * 128, :]
            ticks(pn.a_pre(i, pn.nq + b - 1, pn.nq + pn.blocks), pn.a_pre(i, pn.nq + b, pn.nq + pn.blocks))

    def a_chunk(i, carry):
        for j in range(NC):
            x_copy(i, j).wait()
        norm(i, ga_ref, 0)

        def project(l, carry):
            s = mod(l, DEPTH)
            ahead_a(i, l)

            @pl.when(l < pn.nq - 1)
            def _():
                wait(load_q(l, s))

            @pl.when(l == pn.nq - 1)
            def _():
                wait(load_kv(s))

            acc_s[...] = jnp.dot(abuf[...], wbuf[s], preferred_element_type=f32)

            @pl.when(l < pn.nq - 1)
            def _():
                q_s[l * 2] = turn(acc_s[:, :HEAD])
                q_s[l * 2 + 1] = turn(acc_s[:, HEAD:])

            @pl.when(l == pn.nq - 1)
            def _():
                k_s[...] = turn(acc_s[:, :HEAD])
                v_s[...] = acc_s[:, HEAD:].astype(low)

            ticks(pn.a_pre(i, l - 1, pn.nq + pn.blocks), pn.a_pre(i, l, pn.nq + pn.blocks))
            return carry

        lax.fori_loop(0, pn.nq, project, 0)
        attention(i)

        def out(j, carry):
            g, k = div(j, pn.per), mod(j, pn.per)
            s = mod(g + pn.nq, DEPTH)

            @pl.when(k == 0)
            def _():
                ahead_a(i, g + pn.nq)
                wait(load_o(g, s))

            tile = wbuf[s, pl.ds(pl.multiple_of(k * pn.kq, pn.kq), pn.kq), :]
            acc = jnp.dot(hid[:, : pn.kq], tile, preferred_element_type=f32)
            produce(acc, i * NC + j, j == 0)
            ticks(jnp.where(j == 0, pn.a_pre(i, pn.nq + pn.blocks - 1, pn.nq + pn.blocks), pn.a_wo(i, j - 1)), pn.a_wo(i, j))
            return carry

        lax.fori_loop(0, NC, out, 0)
        combine(i * NC + NC - 1)
        return carry

    def m_chunk(i, carry):
        norm(i, gm_ref, c * H)

        def gated(l, carry):
            s = mod(l, DEPTH)
            ahead_m(i, l)
            wait(load_gu(l, s))
            acc = jnp.dot(abuf[...], wbuf[s], preferred_element_type=f32)
            gate, up = acc[:, :128], acc[:, 128:]
            hid[:, pl.ds(pl.multiple_of(l * 128, 128), 128)] = (gate * (1.0 / (1.0 + jnp.exp(-gate))) * up).astype(low)
            ticks(pn.m_gu(i, l - 1), pn.m_gu(i, l))
            return carry

        lax.fori_loop(0, pn.ng, gated, 0)

        def out(j, carry):
            l = j + pn.ng
            s = mod(l, DEPTH)
            ahead_m(i, l)
            wait(load_d(j, s))
            acc = jnp.dot(hid[...], wbuf[s, : pn.ff, :], preferred_element_type=f32)
            produce(acc, HALF + i * NC + j, j == 0)
            ticks(jnp.where(j == 0, pn.m_gu(i, pn.ng - 1), pn.m_dn(i, j - 1)), pn.m_dn(i, j))
            return carry

        lax.fori_loop(0, NC, out, 0)
        combine(HALF + i * NC + NC - 1)
        return carry

    def x_copy(i, j):
        rows = pl.ds(pl.multiple_of(i * T, T), T)
        return pltpu.make_async_copy(x_ref.at[rows, pl.ds(pl.multiple_of(j * COL, COL), COL)], hbuf.at[j, rows, :], x_sem.at[i, j])

    for j in range(NC):
        x_copy(0, j).start()
    for l in range(DEPTH - 1):
        start_a(jnp.int32(l))

    def more(n, carry):
        x_copy(div(n, NC), mod(n, NC)).start()
        return carry

    lax.fori_loop(NC, pn.seqs * NC, more, 0)

    barrier = pltpu.get_barrier_semaphore()
    for to in (partner, pair):
        pl.semaphore_signal(barrier, inc=1, device_id={"tp": to}, device_id_type=MESH)

    @pl.when(is_mid)
    def _():
        pl.semaphore_signal(barrier, inc=1, device_id={"tp": across}, device_id_type=MESH)
        pl.semaphore_wait(barrier, 3)

    @pl.when(is_end)
    def _():
        pl.semaphore_wait(barrier, 2)

    lax.fori_loop(0, pn.seqs, a_chunk, 0)
    lax.fori_loop(0, pn.seqs, m_chunk, 0)
    done = pn.a_end + pn.km * (pn.seqs - 1) + pn.gu + NC
    ticks(done, NP + pn.lag)

    def drain(s, carry):
        @pl.when(is_end)
        def _():
            z_copy(s).wait_send()

        @pl.when(is_mid)
        def _():
            m_copy(s).wait_send()
            f_copy(s).wait_send()

        g_copy(s).wait_send()
        y_copy(s).wait()
        return carry

    lax.fori_loop(0, UP, drain, 0)
    for s in range(PAIR):
        d_copy(s).wait_send()


def check(pn):
    div_ = lambda a, b: int(a / b) if a < 0 else a // b
    now, made, joined = 0, 0, 0

    def to(n):
        nonlocal now
        now = max(now, n, 0)
        assert now <= joined, (now, joined)

    def make():
        nonlocal made
        assert max(0, now - 2) >= made + 1 - pn.slots, (now, made)
        made += 1

    n = pn.nq + pn.blocks
    for i in range(pn.seqs):
        for k in range(n):
            to(pn.ka * i - pn.offset + div_(pn.before * (k + 1), n))
        for j in range(pn.nc):
            make()
            joined = made - 1
            to(pn.ka * i - pn.offset + pn.before + min(div_(pn.inwo * j + pn.lead, pn.nc), pn.inwo))
        joined = made
    for i in range(pn.seqs):
        assert now >= pn.nc * (i + 1) + pn.lag, (i, now)
        for j in range(pn.ng):
            to(pn.a_end + pn.km * i + div_(pn.gu * (j + 1), pn.ng))
        for j in range(pn.nc):
            make()
            joined = made - 1
            to(pn.a_end + pn.km * i + pn.gu + (j + 1 if i == pn.seqs - 1 else div_(pn.dn * (j + 1), pn.nc)))
        joined = made
    assert made == pn.pieces


def tables(rows):
    half = HEAD // 2
    angle = jnp.arange(rows, dtype=jnp.float32)[:, None] * THETA ** (-jnp.arange(half, dtype=jnp.float32) / half)
    cos, sin = jnp.cos(angle), jnp.sin(angle)
    return jnp.concatenate([cos, cos], 1), jnp.concatenate([-sin, sin], 1)


def layer(x, gain_a, wq, wk, wv, wo, gain_m, w_gate, w_up, w_down):
    seqs, rows, d = x.shape
    pn = Plan(seqs, rows, d, wq.shape[1], w_gate.shape[1])
    check(pn)
    bf, f32, dma = jnp.bfloat16, jnp.float32, pltpu.SemaphoreType.DMA
    far, near = pl.BlockSpec(memory_space=pl.ANY), pl.BlockSpec(memory_space=pltpu.VMEM)
    rc, rs = tables(rows)
    flops = 2 * seqs * rows * (d * (2 * pn.kq + 2 * HEAD) + 3 * d * pn.ff)
    y = pl.pallas_call(
        functools.partial(kernel, pn),
        out_shape=jax.ShapeDtypeStruct((seqs * rows, d), bf),
        in_specs=[far, near, near, near, near] + [far] * 7,
        out_specs=far,
        scratch_shapes=[
            pltpu.VMEM((pn.nc, seqs * rows, COL), bf),
            pltpu.VMEM((rows, d), bf),
            pltpu.VMEM((DEPTH, d, COL), bf),
            pltpu.VMEM((rows, max(pn.ff, pn.kq)), bf),
            pltpu.VMEM((pn.heads, rows, HEAD), bf),
            pltpu.VMEM((rows, HEAD), bf),
            pltpu.VMEM((rows, HEAD), bf),
            pltpu.VMEM((pn.slots, pn.half, COL), f32),
            pltpu.VMEM((PAIR, pn.half, COL), bf),
            pltpu.VMEM((PAIR, pn.half, COL), bf),
            pltpu.VMEM((UP, pn.half, COL), bf),
            pltpu.VMEM((UP, pn.half, COL), bf),
            pltpu.VMEM((UP, pn.half, COL), bf),
            pltpu.VMEM((rows, COL), f32),
            dma((seqs, pn.nc)),
            dma((DEPTH, max(pn.per, 2))),
            dma((UP,)),
            dma((PAIR,)),
            dma((PAIR,)),
            dma((UP,)),
            dma((UP,)),
            dma((UP,)),
            dma((UP,)),
            dma((UP,)),
            dma((UP,)),
            dma((UP,)),
        ],
        compiler_params=pltpu.CompilerParams(collective_id=0, has_side_effects=True, vmem_limit_bytes=63 * 2**20),
        cost_estimate=pl.CostEstimate(flops=flops, transcendentals=0, bytes_accessed=2 * (2 * x.size + wq.size + 3 * w_gate.size)),
    )(x.reshape(seqs * rows, d), gain_a.reshape(1, d), gain_m.reshape(1, d), rc, rs, wq, wk, wv, wo, w_gate, w_up, w_down)
    return y.reshape(x.shape)


def solution(mesh):
    tokens, whole, columns, rows_of = P("dp", None, None), P(None), P(None, "tp"), P("tp", None)
    return jax.shard_map(
        layer,
        mesh=mesh,
        in_specs=(tokens, whole, columns, columns, columns, rows_of, whole, columns, columns, rows_of),
        out_specs=tokens,
        check_vma=False,
    )
```

```python
import functools

import jax
import jax.numpy as jnp
import numpy as np
from jax import lax
from jax.experimental import pallas as pl
from jax.experimental.pallas import tpu as pltpu
from jax.sharding import PartitionSpec as P

HEAD = 128
THETA = 10000
MESH = pl.DeviceIdType.MESH
LOG2E = 1.4426950408889634
HIDDEN = -2e30
COL = 256
UP = 24
PAIR = 16
JOIN = 3
TO_MID, TO_SUM, TO_END, MID_PAIR, END_PAIR = 4, 8, 14, 12, 18
LATE = 3
DEPTH = 3
STRIP = 32


def both(a, b):
    return jnp.logical_and(a, b)


def mod(a, n):
    return lax.rem(a, n)


def div(a, n):
    return lax.div(a, n)


class Plan:
    def __init__(self, seqs, rows, d, kq, ff):
        self.seqs, self.rows, self.d, self.kq, self.ff = seqs, rows, d, kq, ff
        self.half = rows // 2
        self.heads = kq // HEAD
        self.nc = d // COL
        self.units = 4 * seqs * self.nc
        self.nq = kq // COL + 1
        self.per = d // kq
        self.nw = self.nc // self.per
        self.ng = ff // 128
        self.la, self.lm = self.nq + self.nw, self.ng + self.nc
        full = self.nc == 20
        self.first, self.second, self.later, self.gu, self.dn = (
            ((0, 5), (7, 6), (12, 10), 34, 18) if full else ((0, 1), (4, 1), (6, 5), 6, 10))
        self.slots = 94 if full else 44
        self.a0 = sum(self.first) + sum(self.second)
        self.a_end = self.a0 + sum(self.later) * (seqs - 1)
        self.km = self.gu + self.dn
        self.gsteps = self.ng + 2
        self.done = self.a_end + self.km * (seqs - 1) + self.gu + 2 * (self.nc - 1)

    def psteps(self, n):
        return 2 + self.nq + n // 128

    def part(self, which, i):
        if which == 0:
            return (0, *self.first, self.nc - JOIN * self.first[1], 0, self.half)
        if which == 1:
            return (sum(self.first), *self.second, 0, self.half, self.half)
        return (self.a0 + sum(self.later) * (i - 1), *self.later, 0, 0, self.rows)

    def m_gu(self, i, k):
        return self.a_end + self.km * i + div(self.gu * k, self.gsteps)

    def m_dn(self, i, j):
        base = self.a_end + self.km * i + self.gu
        return jnp.where(i == self.seqs - 1, base + 2 * jnp.maximum(j - 1, 0), base + div(self.dn * j, self.nc))


def kernel(pn, x_ref, ga_in, gm_in, rc_in, rs_in, wq_ref, wk_ref, wv_ref, wo_ref, wg_ref, wu_ref, wd_ref, hbuf,
           abuf, wbuf, hid, q_s, k_s, v_s, own, dsend, drecv, usend, zrecv, mrecv, acc_s,
           ga_ref, gm_ref, rc_ref, rs_ref, c_sem, x_sem, w_sem, d_ss, d_rs, u_ss, z_rs, m_rs, f_ss, f_rs, g_ss, g_rs):
    f32, low = jnp.float32, jnp.bfloat16
    T, H, NC, NU, HALF = pn.rows, pn.half, pn.nc, pn.units, pn.units // 2
    t_me = lax.axis_index("tp")
    z, c = div(t_me, 2), mod(t_me, 2)
    is_end = mod(z, 3) == 0
    is_mid = mod(z, 3) != 0
    partner = z * 2 + 1 - c
    pair = (z + 1 - 2 * mod(z, 2)) * 2 + c
    across = (3 - z) * 2 + c

    def remote(src, dst, ss, rs, to):
        return pltpu.make_async_remote_copy(src_ref=src, dst_ref=dst, send_sem=ss, recv_sem=rs, device_id={"tp": to}, device_id_type=MESH)

    def d_copy(s):
        return remote(dsend.at[s], drecv.at[s], d_ss.at[s], d_rs.at[s], partner)

    def z_copy(s):
        return remote(usend.at[s], zrecv.at[s], u_ss.at[s], z_rs.at[s], pair)

    def m_copy(s):
        return remote(usend.at[s], mrecv.at[s], u_ss.at[s], m_rs.at[s], across)

    def mine(u):
        q = mod(u, HALF)
        early = u < 2 * NC
        row = jnp.where(early, div(u, NC) * H, div(q, 2 * NC) * T + mod(q, 2) * H)
        tile = jnp.where(early, mod(u, NC), mod(div(q, 2), NC))
        return hbuf.at[pl.ds(pl.multiple_of(row, H), H), pl.ds(pl.multiple_of(tile * COL + c * 128, 128), 128)]

    def f_copy(u):
        s = mod(u, UP)
        return remote(mine(u), mine(u), f_ss.at[s], f_rs.at[s], pair)

    def g_copy(u):
        s = mod(u, UP)
        return remote(mine(u), mine(u), g_ss.at[s], g_rs.at[s], partner)

    def if_(condition):
        return pl.when(condition)

    def real(u):
        return both(u >= 0, u < NU)

    def leave(u):
        @if_(real(u))
        def _():
            s = mod(u, UP)

            @if_(u >= UP)
            def _():
                z_copy(s).wait_send()

            usend[s] = own[mod(u, pn.slots)].astype(low)
            z_copy(s).start()

    def meet(u):
        @if_(real(u))
        def _():
            s = mod(u, UP)
            z_copy(s).wait_recv()

            @if_(u >= UP)
            def _():
                m_copy(s).wait_send()

            usend[s] = (own[mod(u, pn.slots)] + zrecv[s].astype(f32)).astype(low)
            m_copy(s).start()

    def finish(u):
        @if_(real(u))
        def _():
            s = mod(u, UP)
            m_copy(s).wait_recv()

            @if_(u >= UP)
            def _():
                f_copy(u).wait_send()
                g_copy(u).wait_send()

            to = mine(u)
            to[...] = (to[...].astype(f32) + (usend[s].astype(f32) + mrecv[s].astype(f32))).astype(low)
            f_copy(u).start()
            g_copy(u).start()

    def arrive(u):
        @if_(real(u))
        def _():
            f_copy(u).wait_recv()

            @if_(u >= UP)
            def _():
                g_copy(u).wait_send()

            g_copy(u).start()

    def settle(u):
        @if_(real(u))
        def _():
            g_copy(u).wait_recv()

    def loop(lo, hi, f):
        def one(t, carry):
            f(t)
            return carry

        lax.fori_loop(lo, hi, one, 0)

    def tick(t):
        @if_(is_end)
        def _():
            leave(t)
            arrive(t - TO_END)
            settle(t - END_PAIR)

        @if_(is_mid)
        def _():
            finish(t - TO_SUM)
            meet(t - TO_MID)
            settle(t - MID_PAIR)

    def ticks(lo, hi):
        loop(lo, hi, tick)

    def last_ticks():
        @if_(is_end)
        def _():
            loop(pn.done, NU, tick)

            def rest(u):
                arrive(u)
                settle(u - (END_PAIR - TO_END))

            loop(NU - TO_END, NU + END_PAIR - TO_END, rest)

        @if_(is_mid)
        def _():
            first = pn.done - TO_MID
            loop(pn.done - TO_SUM, first - LATE, finish)

            def rest(u):
                finish(u - LATE)
                meet(u)
                settle(u - (MID_PAIR - TO_MID))

            loop(first, NU + MID_PAIR - TO_MID, rest)

    def combine(u):
        s, o = mod(u, PAIR), mod(u, pn.slots)
        d_copy(s).wait_recv()
        own[o] = own[o] + drecv[s].astype(f32)

    def give(u, acc):
        s = mod(u, PAIR)

        @if_(u >= PAIR)
        def _():
            d_copy(s).wait_send()

        dsend[s] = acc[:, 128:].astype(low)
        own[mod(u, pn.slots)] = acc[:, :128]
        d_copy(s).start()

    def produce(acc, u, j):
        give(u, acc[:H, :])
        give(u + 1, acc[H:, :])

        @if_(j >= JOIN)
        def _():
            combine(u - 2 * JOIN)
            combine(u - 2 * JOIN + 1)

    def produce_first(acc, u, j):
        give(u, acc)

        @if_(j >= JOIN)
        def _():
            combine(u - JOIN)

    def flush(end, n):
        for k in range(n):
            combine(end - n + k)

    def cols(ref, j, n):
        return ref.at[:, pl.ds(pl.multiple_of(j * n, n), n)]

    def load_q(l, s):
        return [pltpu.make_async_copy(cols(wq_ref, l, COL), wbuf.at[s], w_sem.at[s, 0])]

    def load_kv(s):
        return [pltpu.make_async_copy(wk_ref, wbuf.at[s, :, pl.ds(0, HEAD)], w_sem.at[s, 0]),
                pltpu.make_async_copy(wv_ref, wbuf.at[s, :, pl.ds(HEAD, HEAD)], w_sem.at[s, 1])]

    def split(ref, j, to, s, n):
        return [pltpu.make_async_copy(ref.at[:, pl.ds(pl.multiple_of(j * COL + who * 128, 128), 128)], to.at[:, pl.ds(k * 128, 128)],
                                      w_sem.at[s, n + k]) for k, who in enumerate((c, 1 - c))]

    def load_o(l, s):
        return [x for k in range(pn.per) for x in split(wo_ref, l * pn.per + k, wbuf.at[s, pl.ds(k * pn.kq, pn.kq), :], s, 2 * k)]

    def load_gu(l, s):
        return [pltpu.make_async_copy(cols(wg_ref, l, 128), wbuf.at[s, :, pl.ds(0, 128)], w_sem.at[s, 0]),
                pltpu.make_async_copy(cols(wu_ref, l, 128), wbuf.at[s, :, pl.ds(128, 128)], w_sem.at[s, 1])]

    def load_d(l, s):
        return split(wd_ref, l, wbuf.at[s, pl.ds(0, pn.ff), :], s, 0)

    def start(copies):
        for x in copies:
            x.start()

    def wait(copies):
        for x in copies:
            x.wait()

    def start_a(l):
        s = mod(l, DEPTH)

        @pl.when(l < pn.nq - 1)
        def _():
            start(load_q(l, s))

        @pl.when(l == pn.nq - 1)
        def _():
            start(load_kv(s))

        @pl.when(l >= pn.nq)
        def _():
            start(load_o(l - pn.nq, s))

    def start_m(l):
        s = mod(l, DEPTH)

        @pl.when(l < pn.ng)
        def _():
            start(load_gu(l, s))

        @pl.when(l >= pn.ng)
        def _():
            start(load_d(l - pn.ng, s))

    def ahead_a(l, last):
        n = l + DEPTH - 1

        @pl.when(n < pn.la)
        def _():
            start_a(n)

        @pl.when(both(n >= pn.la, jnp.logical_not(last)))
        def _():
            start_a(n - pn.la)

        @pl.when(both(n >= pn.la, last))
        def _():
            start_m(n - pn.la)

    def ahead_m(i, l):
        n = l + DEPTH - 1

        @pl.when(n < pn.lm)
        def _():
            start_m(n)

        @pl.when(both(n >= pn.lm, i < pn.seqs - 1))
        def _():
            start_m(n - pn.lm)

    def gain(g_ref, j):
        return jnp.concatenate([g_ref[k : k + 1, :].astype(f32) for k in range(j * COL // 128, (j + 1) * COL // 128)], axis=1)

    def norm(row, n, g_ref, between):
        def strip(s):
            rows = pl.ds(pl.multiple_of(row + s * STRIP, STRIP), STRIP)
            total = jnp.zeros((STRIP, COL), f32)
            for j in range(NC):
                v = hbuf[rows, j * COL : (j + 1) * COL].astype(f32)
                total += v * v
            scale = lax.rsqrt(jnp.sum(total, axis=-1, keepdims=True) * (1.0 / pn.d) + 1e-6)
            to = pl.ds(pl.multiple_of(s * STRIP, STRIP), STRIP)
            for j in range(NC):
                v = hbuf[rows, j * COL : (j + 1) * COL].astype(f32)
                abuf[to, j * COL : (j + 1) * COL] = (v * scale * gain(g_ref, j)).astype(low)

        def part(k):
            loop(k * (n // STRIP // 2), (k + 1) * (n // STRIP // 2), strip)
            between(k)

        loop(0, 2, part)

    def turn(t, rows):
        t = t.astype(low).astype(f32)
        return (t * rc_ref[rows, :] + pltpu.roll(t, HEAD // 2, 1) * rs_ref[rows, :]).astype(low)

    def attend(b, row):
        e = HEAD**-0.5 * LOG2E
        wide = pn.heads * 128
        gap = mod(lax.broadcasted_iota(jnp.int32, (128, wide), 1), 128) - lax.broadcasted_iota(jnp.int32, (128, wide), 0)
        nk = (b + 1) * 128
        q = q_s[:, b * 128 : (b + 1) * 128, :].reshape(wide, HEAD)
        s = lax.dot_general(k_s[:nk, :], q, (((1,), (1,)), ((), ())), preferred_element_type=f32)
        last = jnp.where(gap >= 0, s[b * 128 :, :], HIDDEN)
        s = last if b == 0 else jnp.concatenate([s[: b * 128, :], last], axis=0)
        p = jnp.exp2((s - s.max(axis=0, keepdims=True)) * e).astype(low)
        values = jnp.concatenate([v_s[:nk, :].T, jnp.ones((8, nk), low)], axis=0)
        o = lax.dot_general(values, p, (((1,), (0,)), ((), ())), preferred_element_type=f32)
        o = (o[:HEAD, :] * (1.0 / o[HEAD : HEAD + 1, :])).T.astype(low)
        to = slice(b * 128 - row, (b + 1) * 128 - row)
        for n in range(pn.heads):
            hid[to, n * HEAD : (n + 1) * HEAD] = o[n * 128 : (n + 1) * 128, :]

    def a_part(which, i, last):
        before, pre, inwo, lead, row, n = pn.part(which, i)
        rows = slice(row, row + n)
        steps = pn.psteps(n)

        def pre_ticks(k):
            if pre or which == 2:
                ticks(before + div(pre * k, steps), before + div(pre * (k + 1), steps))

        def t_wo(j):
            return before + pre + jnp.where(j == NC, inwo, jnp.where(j == 0, 0, div(inwo * (j - 1) + lead, NC)))

        for k in (0, 1) if which == 2 else (which,):
            x_copy(i, k).wait()
        if which == 0:
            for l in range(1, DEPTH - 1):
                start_a(jnp.int32(l))
        if which == 1:
            flush(NC, JOIN)
        if which == 2:
            @if_(i == 1)
            def _():
                flush(2 * NC, JOIN)

            @if_(i > 1)
            def _():
                flush(i * 2 * NC, 2 * JOIN)

        norm(i * T + row, n, ga_ref, pre_ticks)

        def project(l):
            s = mod(l, DEPTH)
            ahead_a(l, last)

            @pl.when(l < pn.nq - 1)
            def _():
                wait(load_q(l, s))

            @pl.when(l == pn.nq - 1)
            def _():
                wait(load_kv(s))

            acc_s[:n, :] = jnp.dot(abuf[:n, :], wbuf[s], preferred_element_type=f32)

            @pl.when(l < pn.nq - 1)
            def _():
                q_s[l * 2, rows, :] = turn(acc_s[:n, :HEAD], rows)
                q_s[l * 2 + 1, rows, :] = turn(acc_s[:n, HEAD:], rows)

            @pl.when(l == pn.nq - 1)
            def _():
                k_s[rows, :] = turn(acc_s[:n, :HEAD], rows)
                v_s[rows, :] = acc_s[:n, HEAD:].astype(low)

            pre_ticks(2 + l)

        loop(0, pn.nq, project)
        if which > 0:
            @if_(i < pn.seqs - 1)
            def _():
                for k in range(2):
                    x_copy(i + 1, k).start()
        for b in range(n // 128):
            attend(row // 128 + b, row)
            pre_ticks(2 + pn.nq + b)

        def out(j):
            g, k = div(j, pn.per), mod(j, pn.per)
            s = mod(g + pn.nq, DEPTH)

            @pl.when(k == 0)
            def _():
                ahead_a(g + pn.nq, last)
                wait(load_o(g, s))

            tile = wbuf[s, pl.ds(pl.multiple_of(k * pn.kq, pn.kq), pn.kq), :]
            acc = jnp.dot(hid[:n, : pn.kq], tile, preferred_element_type=f32)
            if which == 2:
                produce(acc, (i * NC + j) * 2, j)
            else:
                produce_first(acc, which * NC + j, j)
            ticks(t_wo(j), t_wo(j + 1))

        loop(0, NC, out)

    def m_part(i):
        flush(HALF + i * 2 * NC, 2 * JOIN)

        def gu_ticks(k):
            ticks(pn.m_gu(i, k), pn.m_gu(i, k + 1))

        norm(i * T, T, gm_ref, gu_ticks)

        def gated(l):
            s = mod(l, DEPTH)
            ahead_m(i, l)
            wait(load_gu(l, s))
            acc = jnp.dot(abuf[...], wbuf[s], preferred_element_type=f32)
            gate, up = acc[:, :128], acc[:, 128:]
            hid[:, pl.ds(pl.multiple_of(l * 128, 128), 128)] = (gate * (1.0 / (1.0 + jnp.exp(-gate))) * up).astype(low)
            gu_ticks(2 + l)

        loop(0, pn.ng, gated)

        def out(j):
            l = j + pn.ng
            s = mod(l, DEPTH)
            ahead_m(i, l)
            wait(load_d(j, s))
            acc = jnp.dot(hid[...], wbuf[s, : pn.ff, :], preferred_element_type=f32)
            produce(acc, HALF + (i * NC + j) * 2, j)
            ticks(pn.m_dn(i, j), pn.m_dn(i, j + 1))

        loop(0, NC, out)

    def x_copy(i, j):
        at = pl.ds(pl.multiple_of(i * T + j * H, H), H)
        return pltpu.make_async_copy(x_ref.at[at, :], hbuf.at[at, :], x_sem.at[i, j])

    x_copy(0, 0).start()
    start_a(jnp.int32(0))
    small = [pltpu.make_async_copy(a, b, c_sem.at[n])
             for n, (a, b) in enumerate([(ga_in, ga_ref), (rc_in, rc_ref), (rs_in, rs_ref), (gm_in, gm_ref)])]
    start(small)
    x_copy(0, 1).start()

    barrier = pltpu.get_barrier_semaphore()
    for to in (partner, pair):
        pl.semaphore_signal(barrier, inc=1, device_id={"tp": to}, device_id_type=MESH)

    @pl.when(is_mid)
    def _():
        pl.semaphore_signal(barrier, inc=1, device_id={"tp": across}, device_id_type=MESH)
        pl.semaphore_wait(barrier, 3)

    @pl.when(is_end)
    def _():
        pl.semaphore_wait(barrier, 2)

    wait(small)
    a_part(0, 0, False)
    a_part(1, 0, False)
    loop(1, pn.seqs, lambda i: a_part(2, i, i == pn.seqs - 1))
    loop(0, pn.seqs, m_part)
    flush(NU, 2 * JOIN)
    last_ticks()

    def drain(s):
        @if_(is_end)
        def _():
            z_copy(s).wait_send()

        @if_(is_mid)
        def _():
            m_copy(s).wait_send()
            f_copy(s).wait_send()

        g_copy(s).wait_send()

    loop(0, UP, drain)
    loop(0, PAIR, lambda s: d_copy(s).wait_send())


def check(pn):
    now, made, joined = 0, 0, 0

    def to(hi):
        nonlocal now
        assert hi >= now, (hi, now)
        now = hi
        assert now <= joined, (now, joined)

    def make(n):
        nonlocal made
        assert max(0, now - TO_MID) >= made + n - pn.slots, (now, made)
        made += n

    assert pn.la % DEPTH == 0 and pn.lm % DEPTH == 0
    assert UP >= TO_END + 1 - (TO_SUM - TO_MID) and UP >= 2 * (TO_SUM - TO_MID) + 2 and PAIR >= 4 * JOIN + 4
    assert UP > 2 * (MID_PAIR - TO_SUM) + 1 and UP > 2 * (END_PAIR - TO_END) + 1
    for part in range(pn.seqs + 1):
        which = min(part, 2)
        before, pre, inwo, lead, _, n = pn.part(which, part - 1)
        steps = pn.psteps(n)
        joined = made
        assert now == before, (now, before)
        for k in range(steps):
            to(before + pre * (k + 1) // steps)
        for j in range(pn.nc):
            make(2 if which == 2 else 1)
            if j >= JOIN:
                joined = max(joined, made - JOIN * (2 if which == 2 else 1))
            to(before + pre + (inwo if j == pn.nc - 1 else (inwo * j + lead) // pn.nc))
    for i in range(pn.seqs):
        joined = made
        assert now >= 2 * pn.nc * (i + 1) + END_PAIR, (i, now)
        base = pn.a_end + pn.km * i
        assert now == base
        for k in range(pn.gsteps):
            to(base + pn.gu * (k + 1) // pn.gsteps)
        for j in range(pn.nc):
            make(2)
            joined = max(joined, made - 2 * JOIN) if j >= JOIN else joined
            to(base + pn.gu + (2 * j if i == pn.seqs - 1 else pn.dn * (j + 1) // pn.nc))
    assert made == pn.units and now == pn.done


def tables(rows):
    half = HEAD // 2
    angle = np.arange(rows, dtype=np.float32)[:, None] * np.float32(THETA) ** (-np.arange(half, dtype=np.float32) / np.float32(half))
    cos, sin = np.cos(angle), np.sin(angle)
    return np.concatenate([cos, cos], 1), np.concatenate([-sin, sin], 1)


def layer(x, gain_a, wq, wk, wv, wo, gain_m, w_gate, w_up, w_down):
    seqs, rows, d = x.shape
    pn = Plan(seqs, rows, d, wq.shape[1], w_gate.shape[1])
    check(pn)
    bf, f32, dma = jnp.bfloat16, jnp.float32, pltpu.SemaphoreType.DMA
    far = pl.BlockSpec(memory_space=pl.ANY)
    rc, rs = tables(rows)
    flops = 2 * seqs * rows * (d * (2 * pn.kq + 2 * HEAD) + 3 * d * pn.ff)
    y = pl.pallas_call(
        functools.partial(kernel, pn),
        out_shape=pltpu.VMEM((seqs * rows, d), bf),
        in_specs=[far] * 12,
        out_specs=pl.BlockSpec(memory_space=pltpu.VMEM),
        scratch_shapes=[
            pltpu.VMEM((rows, d), bf),
            pltpu.VMEM((DEPTH, d, COL), bf),
            pltpu.VMEM((rows, max(pn.ff, pn.kq)), bf),
            pltpu.VMEM((pn.heads, rows, HEAD), bf),
            pltpu.VMEM((rows, HEAD), bf),
            pltpu.VMEM((rows, HEAD), bf),
            pltpu.VMEM((pn.slots, pn.half, 128), f32),
            pltpu.VMEM((PAIR, pn.half, 128), bf),
            pltpu.VMEM((PAIR, pn.half, 128), bf),
            pltpu.VMEM((UP, pn.half, 128), bf),
            pltpu.VMEM((UP, pn.half, 128), bf),
            pltpu.VMEM((UP, pn.half, 128), bf),
            pltpu.VMEM((rows, COL), f32),
            pltpu.VMEM((d // 128, 128), bf),
            pltpu.VMEM((d // 128, 128), bf),
            pltpu.VMEM((rows, HEAD), f32),
            pltpu.VMEM((rows, HEAD), f32),
            dma((4,)),
            dma((seqs, 2)),
            dma((DEPTH, 2 * pn.per)),
            dma((PAIR,)),
            dma((PAIR,)),
            dma((UP,)),
            dma((UP,)),
            dma((UP,)),
            dma((UP,)),
            dma((UP,)),
            dma((UP,)),
            dma((UP,)),
        ],
        compiler_params=pltpu.CompilerParams(collective_id=0, has_side_effects=True, vmem_limit_bytes=43 * 2**20),
        cost_estimate=pl.CostEstimate(flops=flops, transcendentals=0, bytes_accessed=2 * (2 * x.size + wq.size + 3 * w_gate.size)),
    )(x.reshape(seqs * rows, d), gain_a.reshape(d // 128, 128), gain_m.reshape(d // 128, 128), rc, rs, wq, wk, wv, wo, w_gate, w_up, w_down)
    return y.reshape(x.shape)


def solution(mesh):
    tokens, whole, columns, rows_of = P("dp", None, None), P(None), P(None, "tp"), P("tp", None)
    return jax.shard_map(
        layer,
        mesh=mesh,
        in_specs=(tokens, whole, columns, columns, columns, rows_of, whole, columns, columns, rows_of),
        out_specs=tokens,
        check_vma=False,
    )
```

```python
import functools

import jax
import jax.numpy as jnp
import numpy as np
from jax import lax
from jax.experimental import pallas as pl
from jax.experimental.pallas import tpu as pltpu
from jax.sharding import PartitionSpec as P

HEAD = 128
THETA = 10000
MESH = pl.DeviceIdType.MESH
LOG2E = 1.4426950408889634
HIDDEN = -2e30
COL = 256
UP = 24
PAIR = 16
JOIN = 3
TWOS = 2
TO_MID, TO_SUM, TO_END, MID_PAIR, END_PAIR = 3, 7, 13, 11, 17
LATE = 3
DEPTH = 3
STRIP = 32


def both(a, b):
    return jnp.logical_and(a, b)


def mod(a, n):
    return lax.rem(a, n)


def div(a, n):
    return lax.div(a, n)


class Plan:
    def __init__(self, seqs, rows, d, kq, ff):
        self.seqs, self.rows, self.d, self.kq, self.ff = seqs, rows, d, kq, ff
        self.half = rows // 2
        self.heads = kq // HEAD
        self.nc = d // COL
        self.units = 4 * seqs * self.nc
        self.nq = kq // COL + 1
        self.per = d // kq
        self.nw = self.nc // self.per
        self.ng = ff // 128
        self.la, self.lm = self.nq + self.nw, self.ng + self.nc
        full = self.nc == 20
        self.first, self.second, self.later, self.gu, self.dn = (
            ((0, 0, 0, 6), (2, 5, 2, 5), (3, 8, 3, 7), 34, 18) if full else ((0, 0, 0, 1), (1, 2, 1, 1), (2, 2, 2, 5), 6, 10))
        self.slots = 94 if full else 44
        self.a0 = sum(self.first) + sum(self.second)
        self.a_end = self.a0 + sum(self.later) * (seqs - 1)
        self.km = self.gu + self.dn
        self.gsteps = self.ng + 2
        self.done = self.a_end + self.km * (seqs - 1) + self.gu + 2 * (self.nc - 1)

    def part(self, which, i):
        if which == 0:
            return 0, self.first, 0, 0, self.half
        if which == 1:
            return sum(self.first), self.second, 0, self.half, self.half
        return self.a0 + sum(self.later) * (i - 1), self.later, 0, 0, self.rows

    def m_gu(self, i, k):
        return self.a_end + self.km * i + div(self.gu * k, self.gsteps)

    def m_dn(self, i, j):
        base = self.a_end + self.km * i + self.gu
        return jnp.where(i == self.seqs - 1, base + 2 * jnp.maximum(j - 1, 0), base + div(self.dn * j, self.nc))


def kernel(pn, x_ref, ga_in, gm_in, rc_in, rs_in, wq_ref, wk_ref, wv_ref, wo_ref, wg_ref, wu_ref, wd_ref, hbuf,
           abuf, wbuf, hid, q_s, k_s, v_s, own, dsend, drecv, usend, zrecv, mrecv, acc_s,
           ga_ref, gm_ref, rc_ref, rs_ref, c_sem, x_sem, w_sem, d_ss, d_rs, u_ss, z_rs, m_rs, f_ss, f_rs, g_ss, g_rs):
    f32, low = jnp.float32, jnp.bfloat16
    T, H, NC, NU, HALF = pn.rows, pn.half, pn.nc, pn.units, pn.units // 2
    t_me = lax.axis_index("tp")
    z, c = div(t_me, 2), mod(t_me, 2)
    is_end = mod(z, 3) == 0
    is_mid = mod(z, 3) != 0
    partner = z * 2 + 1 - c
    pair = (z + 1 - 2 * mod(z, 2)) * 2 + c
    across = (3 - z) * 2 + c

    def remote(src, dst, ss, rs, to):
        return pltpu.make_async_remote_copy(src_ref=src, dst_ref=dst, send_sem=ss, recv_sem=rs, device_id={"tp": to}, device_id_type=MESH)

    def d_copy(s):
        return remote(dsend.at[s], drecv.at[s], d_ss.at[s], d_rs.at[s], partner)

    def z_copy(s):
        return remote(usend.at[s], zrecv.at[s], u_ss.at[s], z_rs.at[s], pair)

    def m_copy(s):
        return remote(usend.at[s], mrecv.at[s], u_ss.at[s], m_rs.at[s], across)

    def mine(u):
        q = mod(u, HALF)
        early = u < 2 * NC
        row = jnp.where(early, div(u, NC) * H, div(q, 2 * NC) * T + mod(q, 2) * H)
        tile = jnp.where(early, mod(u, NC), mod(div(q, 2), NC))
        return hbuf.at[pl.ds(pl.multiple_of(row, H), H), pl.ds(pl.multiple_of(tile * COL + c * 128, 128), 128)]

    def f_copy(u):
        s = mod(u, UP)
        return remote(mine(u), mine(u), f_ss.at[s], f_rs.at[s], pair)

    def g_copy(u):
        s = mod(u, UP)
        return remote(mine(u), mine(u), g_ss.at[s], g_rs.at[s], partner)

    def if_(condition):
        return pl.when(condition)

    def real(u):
        return both(u >= 0, u < NU)

    def leave(u):
        @if_(real(u))
        def _():
            s = mod(u, UP)

            @if_(u >= UP)
            def _():
                z_copy(s).wait_send()

            usend[s] = own[mod(u, pn.slots)].astype(low)
            z_copy(s).start()

    def meet(u):
        @if_(real(u))
        def _():
            s = mod(u, UP)
            z_copy(s).wait_recv()

            @if_(u >= UP)
            def _():
                m_copy(s).wait_send()

            usend[s] = (own[mod(u, pn.slots)] + zrecv[s].astype(f32)).astype(low)
            m_copy(s).start()

    def finish(u):
        @if_(real(u))
        def _():
            s = mod(u, UP)
            m_copy(s).wait_recv()

            @if_(u >= UP)
            def _():
                f_copy(u).wait_send()
                g_copy(u).wait_send()

            to = mine(u)
            to[...] = (to[...].astype(f32) + (usend[s].astype(f32) + mrecv[s].astype(f32))).astype(low)
            f_copy(u).start()
            g_copy(u).start()

    def arrive(u):
        @if_(real(u))
        def _():
            f_copy(u).wait_recv()

            @if_(u >= UP)
            def _():
                g_copy(u).wait_send()

            g_copy(u).start()

    def settle(u):
        @if_(real(u))
        def _():
            g_copy(u).wait_recv()

    def loop(lo, hi, f):
        def one(t, carry):
            f(t)
            return carry

        lax.fori_loop(lo, hi, one, 0)

    def tick(t):
        @if_(is_end)
        def _():
            leave(t)
            arrive(t - TO_END)
            settle(t - END_PAIR)

        @if_(is_mid)
        def _():
            finish(t - TO_SUM)
            meet(t - TO_MID)
            settle(t - MID_PAIR)

    def ticks(lo, hi):
        loop(lo, hi, tick)

    def last_ticks():
        @if_(is_end)
        def _():
            loop(pn.done, NU, tick)

            def rest(u):
                arrive(u)
                settle(u - (END_PAIR - TO_END))

            loop(NU - TO_END, NU + END_PAIR - TO_END, rest)

        @if_(is_mid)
        def _():
            first = pn.done - TO_MID
            loop(pn.done - TO_SUM, first - LATE, finish)

            def rest(u):
                finish(u - LATE)
                meet(u)
                settle(u - (MID_PAIR - TO_MID))

            loop(first, NU + MID_PAIR - TO_MID, rest)

    def combine(u):
        s, o = mod(u, PAIR), mod(u, pn.slots)
        d_copy(s).wait_recv()
        own[o] = own[o] + drecv[s].astype(f32)

    def room(u):
        @if_(u >= PAIR)
        def _():
            d_copy(mod(u, PAIR)).wait_send()

    def keep(u, acc):
        dsend[mod(u, PAIR)] = acc[:, 128:].astype(low)
        own[mod(u, pn.slots)] = acc[:, :128]

    def give(u, acc):
        room(u)
        keep(u, acc)
        d_copy(mod(u, PAIR)).start()

    def produce(acc, u, j):
        give(u, acc[:H, :])
        give(u + 1, acc[H:, :])

        @if_(j >= JOIN)
        def _():
            combine(u - 2 * JOIN)
            combine(u - 2 * JOIN + 1)

    def flush(end, n):
        for k in range(n):
            combine(end - n + k)

    def cols(ref, j, n):
        return ref.at[:, pl.ds(pl.multiple_of(j * n, n), n)]

    def load_q(l, s):
        return [pltpu.make_async_copy(cols(wq_ref, l, COL), wbuf.at[s], w_sem.at[s, 0])]

    def load_kv(s):
        return [pltpu.make_async_copy(wk_ref, wbuf.at[s, :, pl.ds(0, HEAD)], w_sem.at[s, 0]),
                pltpu.make_async_copy(wv_ref, wbuf.at[s, :, pl.ds(HEAD, HEAD)], w_sem.at[s, 1])]

    def split(ref, j, to, s, n):
        return [pltpu.make_async_copy(ref.at[:, pl.ds(pl.multiple_of(j * COL + who * 128, 128), 128)], to.at[:, pl.ds(k * 128, 128)],
                                      w_sem.at[s, n + k]) for k, who in enumerate((c, 1 - c))]

    def load_o(l, s):
        return [x for k in range(pn.per) for x in split(wo_ref, l * pn.per + k, wbuf.at[s, pl.ds(k * pn.kq, pn.kq), :], s, 2 * k)]

    def load_gu(l, s):
        return [pltpu.make_async_copy(cols(wg_ref, l, 128), wbuf.at[s, :, pl.ds(0, 128)], w_sem.at[s, 0]),
                pltpu.make_async_copy(cols(wu_ref, l, 128), wbuf.at[s, :, pl.ds(128, 128)], w_sem.at[s, 1])]

    def load_d(l, s):
        return split(wd_ref, l, wbuf.at[s, pl.ds(0, pn.ff), :], s, 0)

    def start(copies):
        for x in copies:
            x.start()

    def wait(copies):
        for x in copies:
            x.wait()

    def start_a(l):
        s = mod(l, DEPTH)

        @pl.when(l < pn.nq - 1)
        def _():
            start(load_q(l, s))

        @pl.when(l == pn.nq - 1)
        def _():
            start(load_kv(s))

        @pl.when(l >= pn.nq)
        def _():
            start(load_o(l - pn.nq, s))

    def start_m(l):
        s = mod(l, DEPTH)

        @pl.when(l < pn.ng)
        def _():
            start(load_gu(l, s))

        @pl.when(l >= pn.ng)
        def _():
            start(load_d(l - pn.ng, s))

    def ahead_a(l, last):
        n = l + DEPTH - 1

        @pl.when(n < pn.la)
        def _():
            start_a(n)

        @pl.when(both(n >= pn.la, jnp.logical_not(last)))
        def _():
            start_a(n - pn.la)

        @pl.when(both(n >= pn.la, last))
        def _():
            start_m(n - pn.la)

    def ahead_m(i, l):
        n = l + DEPTH - 1

        @pl.when(n < pn.lm)
        def _():
            start_m(n)

        @pl.when(both(n >= pn.lm, i < pn.seqs - 1))
        def _():
            start_m(n - pn.lm)

    def gain(g_ref, j):
        return jnp.concatenate([g_ref[k : k + 1, :].astype(f32) for k in range(j * COL // 128, (j + 1) * COL // 128)], axis=1)

    def norm(row, n, g_ref, between):
        def strip(s):
            rows = pl.ds(pl.multiple_of(row + s * STRIP, STRIP), STRIP)
            total = jnp.zeros((STRIP, COL), f32)
            for j in range(NC):
                v = hbuf[rows, j * COL : (j + 1) * COL].astype(f32)
                total += v * v
            scale = lax.rsqrt(jnp.sum(total, axis=-1, keepdims=True) * (1.0 / pn.d) + 1e-6)
            to = pl.ds(pl.multiple_of(s * STRIP, STRIP), STRIP)
            for j in range(NC):
                v = hbuf[rows, j * COL : (j + 1) * COL].astype(f32)
                abuf[to, j * COL : (j + 1) * COL] = (v * scale * gain(g_ref, j)).astype(low)

        def part(k):
            loop(k * (n // STRIP // 2), (k + 1) * (n // STRIP // 2), strip)
            between(k)

        loop(0, 2, part)

    def turn(t, rows):
        t = t.astype(low).astype(f32)
        return (t * rc_ref[rows, :] + pltpu.roll(t, HEAD // 2, 1) * rs_ref[rows, :]).astype(low)

    def attend(b, row):
        e = HEAD**-0.5 * LOG2E
        wide = pn.heads * 128
        gap = mod(lax.broadcasted_iota(jnp.int32, (128, wide), 1), 128) - lax.broadcasted_iota(jnp.int32, (128, wide), 0)
        nk = (b + 1) * 128
        q = q_s[:, b * 128 : (b + 1) * 128, :].reshape(wide, HEAD)
        s = lax.dot_general(k_s[:nk, :], q, (((1,), (1,)), ((), ())), preferred_element_type=f32)
        last = jnp.where(gap >= 0, s[b * 128 :, :], HIDDEN)
        s = last if b == 0 else jnp.concatenate([s[: b * 128, :], last], axis=0)
        p = jnp.exp2((s - s.max(axis=0, keepdims=True)) * e).astype(low)
        values = jnp.concatenate([v_s[:nk, :].T, jnp.ones((8, nk), low)], axis=0)
        o = lax.dot_general(values, p, (((1,), (0,)), ((), ())), preferred_element_type=f32)
        o = (o[:HEAD, :] * (1.0 / o[HEAD : HEAD + 1, :])).T.astype(low)
        to = slice(b * 128 - row, (b + 1) * 128 - row)
        for n in range(pn.heads):
            hid[to, n * HEAD : (n + 1) * HEAD] = o[n * 128 : (n + 1) * 128, :]

    def a_part(which, i, last):
        before, (c_norm, c_proj, c_att, c_wo), lead, row, n = pn.part(which, i)
        rows = slice(row, row + n)

        def share(before, count, k, steps):
            if count:
                ticks(before + div(count * k, steps), before + div(count * (k + 1), steps))

        b_proj = before + c_norm
        b_att = b_proj + c_proj
        b_wo = b_att + c_att

        def t_wo(j):
            return b_wo + jnp.where(j == NC // 2, c_wo, jnp.where(j == 0, 0, div(c_wo * (j - 1) + lead, NC // 2)))

        for k in (0, 1) if which == 2 else (which,):
            x_copy(i, k).wait()
        if which == 0:
            for l in range(1, DEPTH - 1):
                start_a(jnp.int32(l))
        if which == 1:
            flush(NC, 2 * TWOS)
        if which == 2:
            @if_(i == 1)
            def _():
                flush(2 * NC, 2 * TWOS)

            @if_(i > 1)
            def _():
                flush(i * 2 * NC, 4 * TWOS)

        norm(i * T + row, n, ga_ref, lambda k: share(before, c_norm, k, 2))

        def project(l):
            s = mod(l, DEPTH)
            ahead_a(l, last)

            @pl.when(l < pn.nq - 1)
            def _():
                wait(load_q(l, s))

            @pl.when(l == pn.nq - 1)
            def _():
                wait(load_kv(s))

            acc_s[:n, :] = jnp.dot(abuf[:n, :], wbuf[s], preferred_element_type=f32)

            @pl.when(l < pn.nq - 1)
            def _():
                q_s[l * 2, rows, :] = turn(acc_s[:n, :HEAD], rows)
                q_s[l * 2 + 1, rows, :] = turn(acc_s[:n, HEAD:], rows)

            @pl.when(l == pn.nq - 1)
            def _():
                k_s[rows, :] = turn(acc_s[:n, :HEAD], rows)
                v_s[rows, :] = acc_s[:n, HEAD:].astype(low)

            share(b_proj, c_proj, l, pn.nq)

        loop(0, pn.nq, project)
        if which > 0:
            @if_(i < pn.seqs - 1)
            def _():
                for k in range(2):
                    x_copy(i + 1, k).start()
        for b in range(n // 128):
            attend(row // 128 + b, row)
            share(b_att, c_att, b, n // 128)

        base, each = (i * 2 * NC, 4) if which == 2 else (which * NC, 2)

        def out(j):
            tiles = [(div(t, pn.per), mod(t, pn.per)) for t in (2 * j, 2 * j + 1)]
            u = base + j * each
            for g, k in tiles:
                @if_(k == 0)
                def _():
                    wait(load_o(g, mod(g + pn.nq, DEPTH)))

            for n_ in range(each):
                room(u + n_)
            for t, (g, k) in enumerate(tiles):
                tile = wbuf[mod(g + pn.nq, DEPTH), pl.ds(pl.multiple_of(k * pn.kq, pn.kq), pn.kq), :]
                acc = jnp.dot(hid[:n, : pn.kq], tile, preferred_element_type=f32)
                for n_ in range(each // 2):
                    keep(u + t * (each // 2) + n_, acc[n_ * H : (n_ + 1) * H, :])
            for g, k in tiles:
                @if_(k == 0)
                def _():
                    ahead_a(g + pn.nq, last)

            @if_(j >= TWOS)
            def _():
                for n_ in range(each):
                    combine(u - TWOS * each + n_)

            for n_ in range(each):
                d_copy(mod(u + n_, PAIR)).start()
            ticks(t_wo(j), t_wo(j + 1))

        loop(0, NC // 2, out)

    def m_part(i):
        @if_(i == 0)
        def _():
            flush(HALF, 4 * TWOS)

        @if_(i > 0)
        def _():
            flush(HALF + i * 2 * NC, 2 * JOIN)

        def gu_ticks(k):
            ticks(pn.m_gu(i, k), pn.m_gu(i, k + 1))

        norm(i * T, T, gm_ref, gu_ticks)

        def gated(l):
            s = mod(l, DEPTH)
            ahead_m(i, l)
            wait(load_gu(l, s))
            acc = jnp.dot(abuf[...], wbuf[s], preferred_element_type=f32)
            gate, up = acc[:, :128], acc[:, 128:]
            hid[:, pl.ds(pl.multiple_of(l * 128, 128), 128)] = (gate * (1.0 / (1.0 + jnp.exp(-gate))) * up).astype(low)
            gu_ticks(2 + l)

        loop(0, pn.ng, gated)

        def out(j):
            l = j + pn.ng
            s = mod(l, DEPTH)
            ahead_m(i, l)
            wait(load_d(j, s))
            acc = jnp.dot(hid[...], wbuf[s, : pn.ff, :], preferred_element_type=f32)
            produce(acc, HALF + (i * NC + j) * 2, j)
            ticks(pn.m_dn(i, j), pn.m_dn(i, j + 1))

        loop(0, NC, out)

    def x_copy(i, j):
        at = pl.ds(pl.multiple_of(i * T + j * H, H), H)
        return pltpu.make_async_copy(x_ref.at[at, :], hbuf.at[at, :], x_sem.at[i, j])

    x_copy(0, 0).start()
    start_a(jnp.int32(0))
    small = [pltpu.make_async_copy(a, b, c_sem.at[n])
             for n, (a, b) in enumerate([(ga_in, ga_ref), (rc_in, rc_ref), (rs_in, rs_ref), (gm_in, gm_ref)])]
    start(small)
    x_copy(0, 1).start()

    barrier = pltpu.get_barrier_semaphore()
    for to in (partner, pair):
        pl.semaphore_signal(barrier, inc=1, device_id={"tp": to}, device_id_type=MESH)

    @pl.when(is_mid)
    def _():
        pl.semaphore_signal(barrier, inc=1, device_id={"tp": across}, device_id_type=MESH)
        pl.semaphore_wait(barrier, 3)

    @pl.when(is_end)
    def _():
        pl.semaphore_wait(barrier, 2)

    wait(small)
    a_part(0, 0, False)
    a_part(1, 0, False)
    loop(1, pn.seqs, lambda i: a_part(2, i, i == pn.seqs - 1))
    loop(0, pn.seqs, m_part)
    flush(NU, 2 * JOIN)
    last_ticks()

    def drain(s):
        @if_(is_end)
        def _():
            z_copy(s).wait_send()

        @if_(is_mid)
        def _():
            m_copy(s).wait_send()
            f_copy(s).wait_send()

        g_copy(s).wait_send()

    loop(0, UP, drain)
    loop(0, PAIR, lambda s: d_copy(s).wait_send())


def check(pn):
    now, made, joined = 0, 0, 0

    def to(hi):
        nonlocal now
        assert hi >= now, (hi, now)
        now = hi
        assert now <= joined, (now, joined)

    def make(n):
        nonlocal made
        assert max(0, now - TO_MID) >= made + n - pn.slots, (now, made)
        made += n

    assert pn.la % DEPTH == 0 and pn.lm % DEPTH == 0
    assert UP >= TO_END + 1 - (TO_SUM - TO_MID) and UP >= 2 * (TO_SUM - TO_MID) + 2 and PAIR >= 4 * JOIN + 4 and PAIR >= 8 * TWOS
    assert UP > 2 * (MID_PAIR - TO_SUM) + 1 and UP > 2 * (END_PAIR - TO_END) + 1
    for part in range(pn.seqs + 1):
        which = min(part, 2)
        before, counts, lead, _, n = pn.part(which, part - 1)
        joined = made
        assert now == before, (now, before)
        for count, steps in zip(counts, (2, pn.nq, n // 128)):
            at = now
            for k in range(steps):
                to(at + count * (k + 1) // steps)
        at, inwo = now, counts[3]
        each = 4 if which == 2 else 2
        for j in range(pn.nc // 2):
            make(each)
            joined = made - TWOS * each if j >= TWOS else joined
            to(at + (inwo if j == pn.nc // 2 - 1 else (inwo * j + lead) // (pn.nc // 2)))
    for i in range(pn.seqs):
        joined = made
        assert now >= 2 * pn.nc * (i + 1) + END_PAIR, (i, now)
        base = pn.a_end + pn.km * i
        assert now == base
        for k in range(pn.gsteps):
            to(base + pn.gu * (k + 1) // pn.gsteps)
        for j in range(pn.nc):
            make(2)
            joined = max(joined, made - 2 * JOIN) if j >= JOIN else joined
            to(base + pn.gu + (2 * j if i == pn.seqs - 1 else pn.dn * (j + 1) // pn.nc))
    assert made == pn.units and now == pn.done


def tables(rows):
    half = HEAD // 2
    angle = np.arange(rows, dtype=np.float32)[:, None] * np.float32(THETA) ** (-np.arange(half, dtype=np.float32) / np.float32(half))
    cos, sin = np.cos(angle), np.sin(angle)
    return np.concatenate([cos, cos], 1), np.concatenate([-sin, sin], 1)


def layer(x, gain_a, wq, wk, wv, wo, gain_m, w_gate, w_up, w_down):
    seqs, rows, d = x.shape
    pn = Plan(seqs, rows, d, wq.shape[1], w_gate.shape[1])
    check(pn)
    bf, f32, dma = jnp.bfloat16, jnp.float32, pltpu.SemaphoreType.DMA
    far = pl.BlockSpec(memory_space=pl.ANY)
    rc, rs = tables(rows)
    flops = 2 * seqs * rows * (d * (2 * pn.kq + 2 * HEAD) + 3 * d * pn.ff)
    y = pl.pallas_call(
        functools.partial(kernel, pn),
        out_shape=pltpu.VMEM((seqs * rows, d), bf),
        in_specs=[far] * 12,
        out_specs=pl.BlockSpec(memory_space=pltpu.VMEM),
        scratch_shapes=[
            pltpu.VMEM((rows, d), bf),
            pltpu.VMEM((DEPTH, d, COL), bf),
            pltpu.VMEM((rows, max(pn.ff, pn.kq)), bf),
            pltpu.VMEM((pn.heads, rows, HEAD), bf),
            pltpu.VMEM((rows, HEAD), bf),
            pltpu.VMEM((rows, HEAD), bf),
            pltpu.VMEM((pn.slots, pn.half, 128), f32),
            pltpu.VMEM((PAIR, pn.half, 128), bf),
            pltpu.VMEM((PAIR, pn.half, 128), bf),
            pltpu.VMEM((UP, pn.half, 128), bf),
            pltpu.VMEM((UP, pn.half, 128), bf),
            pltpu.VMEM((UP, pn.half, 128), bf),
            pltpu.VMEM((rows, COL), f32),
            pltpu.VMEM((d // 128, 128), bf),
            pltpu.VMEM((d // 128, 128), bf),
            pltpu.VMEM((rows, HEAD), f32),
            pltpu.VMEM((rows, HEAD), f32),
            dma((4,)),
            dma((seqs, 2)),
            dma((DEPTH, 2 * pn.per)),
            dma((PAIR,)),
            dma((PAIR,)),
            dma((UP,)),
            dma((UP,)),
            dma((UP,)),
            dma((UP,)),
            dma((UP,)),
            dma((UP,)),
            dma((UP,)),
        ],
        compiler_params=pltpu.CompilerParams(collective_id=0, has_side_effects=True, vmem_limit_bytes=43 * 2**20),
        cost_estimate=pl.CostEstimate(flops=flops, transcendentals=0, bytes_accessed=2 * (2 * x.size + wq.size + 3 * w_gate.size)),
    )(x.reshape(seqs * rows, d), gain_a.reshape(d // 128, 128), gain_m.reshape(d // 128, 128), rc, rs, wq, wk, wv, wo, w_gate, w_up, w_down)
    return y.reshape(x.shape)


def solution(mesh):
    tokens, whole, columns, rows_of = P("dp", None, None), P(None), P(None, "tp"), P("tp", None)
    return jax.shard_map(
        layer,
        mesh=mesh,
        in_specs=(tokens, whole, columns, columns, columns, rows_of, whole, columns, columns, rows_of),
        out_specs=tokens,
        check_vma=False,
    )
```

```python
import functools

import jax
import jax.numpy as jnp
import numpy as np
from jax import lax
from jax.experimental import pallas as pl
from jax.experimental.pallas import tpu as pltpu
from jax.sharding import PartitionSpec as P

HEAD = 128
THETA = 10000
MESH = pl.DeviceIdType.MESH
LOG2E = 1.4426950408889634
HIDDEN = -2e30
COL = 256
UP = 24
PAIR = 16
JOIN = 3
TWOS = 2
TO_MID, TO_SUM, TO_END, MID_PAIR, END_PAIR = 3, 7, 13, 11, 17
LATE = 3
DEPTH = 3
STRIP = 32
PARTS = 4
OUT = 8
XCUT = 8


def both(a, b):
    return jnp.logical_and(a, b)


def mod(a, n):
    return lax.rem(a, n)


def div(a, n):
    return lax.div(a, n)


class Plan:
    def __init__(self, seqs, rows, d, kq, ff):
        self.seqs, self.rows, self.d, self.kq, self.ff = seqs, rows, d, kq, ff
        self.half = rows // 2
        self.heads = kq // HEAD
        self.nc = d // COL
        self.units = 4 * seqs * self.nc
        self.nq = kq // COL + 1
        self.per = d // kq
        self.nw = self.nc // self.per
        self.ng = ff // 128
        self.la, self.lm = self.nq + self.nw, self.ng + self.nc
        full = self.nc == 20
        self.first, self.second, self.later, (self.mn, self.gu, self.dn) = (
            ((0, 0, 0, 6), (2, 5, 2, 5), (3, 7, 3, 9), (3, 31, 18)) if full else ((0, 0, 0, 1), (1, 2, 1, 1), (2, 2, 2, 5), (2, 4, 10)))
        self.slots = 94 if full else 44
        self.a0 = sum(self.first) + sum(self.second)
        self.a_end = self.a0 + sum(self.later) * (seqs - 1)
        self.km = self.mn + self.gu + self.dn
        self.done = self.a_end + self.km * (seqs - 1) + self.mn + self.gu + 2 * (self.nc - 1)

    def part(self, which, i):
        if which == 0:
            return 0, self.first, 0, 0, self.half
        if which == 1:
            return sum(self.first), self.second, 0, self.half, self.half
        return self.a0 + sum(self.later) * (i - 1), self.later, 0, 0, self.rows

    def m_norm(self, i):
        return self.a_end + self.km * i

    def m_dn(self, i, j):
        base = self.m_norm(i) + self.mn + self.gu
        return jnp.where(i == self.seqs - 1, base + 2 * jnp.maximum(j - 1, 0), base + div(self.dn * j, self.nc))


def kernel(pn, x_ref, ga_in, gm_in, rc_in, rs_in, wq_ref, wk_ref, wv_ref, wo_ref, wg_ref, wu_ref, wd_ref, hbuf,
           abuf, wbuf, hid, q_s, k_s, v_s, own, dsend, drecv, usend, zrecv, mrecv, acc_s,
           ga_ref, gm_ref, rc_ref, rs_ref, c_sem, x_sem, w_sem, d_ss, d_rs, u_ss, z_rs, m_rs, f_ss, f_rs, g_ss, g_rs):
    f32, low = jnp.float32, jnp.bfloat16
    T, H, NC, NU, HALF = pn.rows, pn.half, pn.nc, pn.units, pn.units // 2
    t_me = lax.axis_index("tp")
    z, c = div(t_me, 2), mod(t_me, 2)
    is_end = mod(z, 3) == 0
    is_mid = mod(z, 3) != 0
    partner = z * 2 + 1 - c
    pair = (z + 1 - 2 * mod(z, 2)) * 2 + c
    across = (3 - z) * 2 + c

    def remote(src, dst, ss, rs, to):
        return pltpu.make_async_remote_copy(src_ref=src, dst_ref=dst, send_sem=ss, recv_sem=rs, device_id={"tp": to}, device_id_type=MESH)

    def d_copy(s):
        return remote(dsend.at[s], drecv.at[s], d_ss.at[s], d_rs.at[s], partner)

    def z_copy(s):
        return remote(usend.at[s], zrecv.at[s], u_ss.at[s], z_rs.at[s], pair)

    def m_copy(s):
        return remote(usend.at[s], mrecv.at[s], u_ss.at[s], m_rs.at[s], across)

    def mine(u):
        q = mod(u, HALF)
        early = u < 2 * NC
        row = jnp.where(early, div(u, NC) * H, div(q, 2 * NC) * T + mod(q, 2) * H)
        tile = jnp.where(early, mod(u, NC), mod(div(q, 2), NC))
        return hbuf.at[pl.ds(pl.multiple_of(row, H), H), pl.ds(pl.multiple_of(tile * COL + c * 128, 128), 128)]

    def f_copy(u):
        s = mod(u, UP)
        return remote(mine(u), mine(u), f_ss.at[s], f_rs.at[s], pair)

    def g_copy(u):
        s = mod(u, UP)
        return remote(mine(u), mine(u), g_ss.at[s], g_rs.at[s], partner)

    def if_(condition):
        return pl.when(condition)

    def real(u, steady):
        return (lambda f: f()) if steady else if_(both(u >= 0, u < NU))

    def old(u, n, steady):
        return (lambda f: f()) if steady else if_(u >= n)

    def leave(u, steady=False):
        @real(u, steady)
        def _():
            s = mod(u, UP)

            @old(u, UP, steady)
            def _():
                z_copy(s).wait_send()

            usend[s] = own[mod(u, pn.slots)].astype(low)
            z_copy(s).start()

    def meet(u, steady=False):
        @real(u, steady)
        def _():
            s = mod(u, UP)
            z_copy(s).wait_recv()

            @old(u, UP, steady)
            def _():
                m_copy(s).wait_send()

            usend[s] = (own[mod(u, pn.slots)] + zrecv[s].astype(f32)).astype(low)
            m_copy(s).start()

    def finish(u, steady=False):
        @real(u, steady)
        def _():
            s = mod(u, UP)
            m_copy(s).wait_recv()

            @old(u, UP, steady)
            def _():
                f_copy(u).wait_send()
                g_copy(u).wait_send()

            to = mine(u)
            to[...] = (to[...].astype(f32) + (usend[s].astype(f32) + mrecv[s].astype(f32))).astype(low)
            f_copy(u).start()
            g_copy(u).start()

    def arrive(u, steady=False):
        @real(u, steady)
        def _():
            f_copy(u).wait_recv()

            @old(u, UP, steady)
            def _():
                g_copy(u).wait_send()

            g_copy(u).start()

    def settle(u, steady=False):
        @real(u, steady)
        def _():
            g_copy(u).wait_recv()

    def loop(lo, hi, f):
        def one(t, carry):
            f(t)
            return carry

        lax.fori_loop(lo, hi, one, 0)

    def tick(t, steady=False):
        @if_(is_end)
        def _():
            leave(t, steady)
            arrive(t - TO_END, steady)
            settle(t - END_PAIR, steady)

        @if_(is_mid)
        def _():
            finish(t - TO_SUM, steady)
            meet(t - TO_MID, steady)
            settle(t - MID_PAIR, steady)

    def ticks(lo, hi, steady=False):
        loop(lo, hi, lambda t: tick(t, steady))

    def last_ticks():
        @if_(is_end)
        def _():
            loop(pn.done, NU, tick)
            early = UP - TO_END - 2

            def rest(u):
                arrive(u)
                settle(u - (END_PAIR - TO_END))
                n = u - (NU - TO_END)

                @if_(n < early)
                def _():
                    for k in range(2):
                        g_copy(NU - UP + 2 * n + k).wait_send()

                @if_(u == NU - 3)
                def _():
                    loop(0, UP, lambda s: z_copy(s).wait_send())

            loop(NU - TO_END, NU + END_PAIR - TO_END, rest)
            loop(NU - UP + 2 * early, NU, lambda u: g_copy(u).wait_send())

        @if_(is_mid)
        def _():
            first = pn.done - TO_MID
            loop(pn.done - TO_SUM, first - LATE, finish)

            def rest(u):
                finish(u - LATE)
                meet(u)
                settle(u - (MID_PAIR - TO_MID))

            loop(first, NU + MID_PAIR - TO_MID, rest)

            def drain(s):
                m_copy(s).wait_send()
                f_copy(s).wait_send()
                g_copy(s).wait_send()

            loop(0, UP, drain)

    def combine(u):
        s, o = mod(u, PAIR), mod(u, pn.slots)
        d_copy(s).wait_recv()
        own[o] = own[o] + drecv[s].astype(f32)

    def room(u, steady=False):
        @old(u, PAIR, steady)
        def _():
            d_copy(mod(u, PAIR)).wait_send()

    def keep(u, acc):
        dsend[mod(u, PAIR)] = acc[:, 128:].astype(low)
        own[mod(u, pn.slots)] = acc[:, :128]

    def give(u, acc):
        room(u, True)
        keep(u, acc)
        d_copy(mod(u, PAIR)).start()

    def produce(acc, u, j):
        give(u, acc[:H, :])
        give(u + 1, acc[H:, :])

        @if_(j >= JOIN)
        def _():
            combine(u - 2 * JOIN)
            combine(u - 2 * JOIN + 1)

    def flush(end, n):
        for k in range(n):
            combine(end - n + k)

    def cols(ref, j, n):
        return ref.at[:, pl.ds(pl.multiple_of(j * n, n), n)]

    def load_q(l, s):
        return [pltpu.make_async_copy(cols(wq_ref, l, COL), wbuf.at[s], w_sem.at[s, 0])]

    def load_kv(s):
        return [pltpu.make_async_copy(wk_ref, wbuf.at[s, :, pl.ds(0, HEAD)], w_sem.at[s, 0]),
                pltpu.make_async_copy(wv_ref, wbuf.at[s, :, pl.ds(HEAD, HEAD)], w_sem.at[s, 1])]

    def split(ref, j, to, s, n):
        return [pltpu.make_async_copy(ref.at[:, pl.ds(pl.multiple_of(j * COL + who * 128, 128), 128)], to.at[:, pl.ds(k * 128, 128)],
                                      w_sem.at[s, n + k]) for k, who in enumerate((c, 1 - c))]

    def load_o(l, s):
        return [x for k in range(pn.per) for x in split(wo_ref, l * pn.per + k, wbuf.at[s, pl.ds(k * pn.kq, pn.kq), :], s, 2 * k)]

    def load_gu(l, s):
        return [pltpu.make_async_copy(cols(wg_ref, l, 128), wbuf.at[s, :, pl.ds(0, 128)], w_sem.at[s, 0]),
                pltpu.make_async_copy(cols(wu_ref, l, 128), wbuf.at[s, :, pl.ds(128, 128)], w_sem.at[s, 1])]

    def load_d(l, s):
        return split(wd_ref, l, wbuf.at[s, pl.ds(0, pn.ff), :], s, 0)

    def start(copies):
        for x in copies:
            x.start()

    def wait(copies):
        for x in copies:
            x.wait()

    def start_a(l):
        s = mod(l, DEPTH)

        @pl.when(l < pn.nq - 1)
        def _():
            start(load_q(l, s))

        @pl.when(l == pn.nq - 1)
        def _():
            start(load_kv(s))

        @pl.when(l >= pn.nq)
        def _():
            start(load_o(l - pn.nq, s))

    def start_m(l):
        s = mod(l, DEPTH)

        @pl.when(l < pn.ng)
        def _():
            start(load_gu(l, s))

        @pl.when(l >= pn.ng)
        def _():
            start(load_d(l - pn.ng, s))

    def ahead_a(l, last):
        n = l + DEPTH - 1

        @pl.when(n < pn.la)
        def _():
            start_a(n)

        @pl.when(both(n >= pn.la, jnp.logical_not(last)))
        def _():
            start_a(n - pn.la)

        @pl.when(both(n >= pn.la, last))
        def _():
            start_m(n - pn.la)

    def ahead_m(i, l):
        n = l + DEPTH - 1

        @pl.when(n < pn.lm)
        def _():
            start_m(n)

        @pl.when(both(n >= pn.lm, i < pn.seqs - 1))
        def _():
            start_m(n - pn.lm)

    def gain(g_ref, j):
        return jnp.concatenate([g_ref[k : k + 1, :].astype(f32) for k in range(j * COL // 128, (j + 1) * COL // 128)], axis=1)

    def norm(row, n, g_ref, between, early, come=None):
        cut = n // STRIP // PARTS

        def strip(s):
            rows = pl.ds(pl.multiple_of(row + s * STRIP, STRIP), STRIP)
            total = jnp.zeros((STRIP, COL), f32)
            for j in range(NC):
                v = hbuf[rows, j * COL : (j + 1) * COL].astype(f32)
                total += v * v
            scale = lax.rsqrt(jnp.sum(total, axis=-1, keepdims=True) * (1.0 / pn.d) + 1e-6)
            to = pl.ds(pl.multiple_of(s * STRIP, STRIP), STRIP)
            for j in range(NC):
                v = hbuf[rows, j * COL : (j + 1) * COL].astype(f32)
                abuf[to, j * COL : (j + 1) * COL] = (v * scale * gain(g_ref, j)).astype(low)

        def part(k):
            if come is not None:
                come(k)
            loop(k * cut, (k + 1) * cut, strip)
            between(k)

        part(0)
        early()
        loop(1, PARTS, part)

    def turn(t, rows):
        t = t.astype(low).astype(f32)
        return (t * rc_ref[rows, :] + pltpu.roll(t, HEAD // 2, 1) * rs_ref[rows, :]).astype(low)

    def attend(b, row):
        e = HEAD**-0.5 * LOG2E
        wide = pn.heads * 128
        gap = mod(lax.broadcasted_iota(jnp.int32, (128, wide), 1), 128) - lax.broadcasted_iota(jnp.int32, (128, wide), 0)
        nk = (b + 1) * 128
        q = q_s[:, b * 128 : (b + 1) * 128, :].reshape(wide, HEAD)
        s = lax.dot_general(k_s[:nk, :], q, (((1,), (1,)), ((), ())), preferred_element_type=f32)
        last = jnp.where(gap >= 0, s[b * 128 :, :], HIDDEN)
        s = last if b == 0 else jnp.concatenate([s[: b * 128, :], last], axis=0)
        p = jnp.exp2((s - s.max(axis=0, keepdims=True)) * e).astype(low)
        values = jnp.concatenate([v_s[:nk, :].T, jnp.ones((8, nk), low)], axis=0)
        o = lax.dot_general(values, p, (((1,), (0,)), ((), ())), preferred_element_type=f32)
        o = (o[:HEAD, :] * (1.0 / o[HEAD : HEAD + 1, :])).T.astype(low)
        to = slice(b * 128 - row, (b + 1) * 128 - row)
        for n in range(pn.heads):
            hid[to, n * HEAD : (n + 1) * HEAD] = o[n * 128 : (n + 1) * 128, :]

    def share(before, count, k, steps, steady=False):
        if count:
            ticks(before + div(count * k, steps), before + div(count * (k + 1), steps), steady)

    def a_part(which, i, last):
        before, (c_norm, c_proj, c_att, c_wo), lead, row, n = pn.part(which, i)
        rows = slice(row, row + n)

        b_proj = before + c_norm
        b_att = b_proj + c_proj
        b_wo = b_att + c_att

        def t_wo(j):
            return b_wo + jnp.where(j == NC // 2, c_wo, jnp.where(j == 0, 0, div(c_wo * (j - 1) + lead, NC // 2)))

        if which == 0:
            wait(small[:1])

        def early():
            if which == 0:
                for l in range(1, DEPTH - 1):
                    start_a(jnp.int32(l))
            if which == 1:
                flush(NC, 2 * TWOS)
            if which == 2:
                @if_(i == 1)
                def _():
                    flush(2 * NC, 2 * TWOS)

                @if_(i > 1)
                def _():
                    flush(i * 2 * NC, 4 * TWOS)

        each = n * XCUT // T // PARTS

        def come(k):
            for m in range(each):
                x_copy(i, row * XCUT // T + k * each + m).wait()

        norm(i * T + row, n, ga_ref, lambda k: share(before, c_norm, k, PARTS), early, come)
        if which == 0:
            wait(small[1:])

        def project(l):
            s = mod(l, DEPTH)
            ahead_a(l, last)

            @pl.when(l < pn.nq - 1)
            def _():
                wait(load_q(l, s))

            @pl.when(l == pn.nq - 1)
            def _():
                wait(load_kv(s))

            acc_s[:n, :] = jnp.dot(abuf[:n, :], wbuf[s], preferred_element_type=f32)

            @pl.when(l < pn.nq - 1)
            def _():
                q_s[l * 2, rows, :] = turn(acc_s[:n, :HEAD], rows)
                q_s[l * 2 + 1, rows, :] = turn(acc_s[:n, HEAD:], rows)

            @pl.when(l == pn.nq - 1)
            def _():
                k_s[rows, :] = turn(acc_s[:n, :HEAD], rows)
                v_s[rows, :] = acc_s[:n, HEAD:].astype(low)

            share(b_proj, c_proj, l, pn.nq)

        loop(0, pn.nq, project)
        if which > 0:
            @if_(i < pn.seqs - 1)
            def _():
                for k in range(XCUT):
                    x_copy(i + 1, k).start()
        for b in range(n // 128):
            attend(row // 128 + b, row)
            share(b_att, c_att, b, n // 128)

        if which == 0:
            greeted()
        base, each = (i * 2 * NC, 4) if which == 2 else (which * NC, 2)

        def out(j):
            tiles = [(div(t, pn.per), mod(t, pn.per)) for t in (2 * j, 2 * j + 1)]
            u = base + j * each
            for g, k in tiles:
                @if_(k == 0)
                def _():
                    wait(load_o(g, mod(g + pn.nq, DEPTH)))

            for n_ in range(each):
                room(u + n_)
            for t, (g, k) in enumerate(tiles):
                tile = wbuf[mod(g + pn.nq, DEPTH), pl.ds(pl.multiple_of(k * pn.kq, pn.kq), pn.kq), :]
                acc = jnp.dot(hid[:n, : pn.kq], tile, preferred_element_type=f32)
                for n_ in range(each // 2):
                    keep(u + t * (each // 2) + n_, acc[n_ * H : (n_ + 1) * H, :])
            for g, k in tiles:
                @if_(k == 0)
                def _():
                    ahead_a(g + pn.nq, last)

            @if_(j >= TWOS)
            def _():
                for n_ in range(each):
                    combine(u - TWOS * each + n_)

            for n_ in range(each):
                d_copy(mod(u + n_, PAIR)).start()
            ticks(t_wo(j), t_wo(j + 1))

        loop(0, NC // 2, out)

    def m_part(i):
        def early():
            @if_(i == 0)
            def _():
                flush(HALF, 4 * TWOS)

            @if_(i > 0)
            def _():
                flush(HALF + i * 2 * NC, 2 * JOIN)

        base = pn.m_norm(i)
        norm(i * T, T, gm_ref, lambda k: share(base, pn.mn, k, PARTS, True), early)

        def gated(l):
            s = mod(l, DEPTH)
            ahead_m(i, l)
            wait(load_gu(l, s))
            acc = jnp.dot(abuf[...], wbuf[s], preferred_element_type=f32)
            gate, up = acc[:, :128], acc[:, 128:]
            hid[:, pl.ds(pl.multiple_of(l * 128, 128), 128)] = (gate * (1.0 / (1.0 + jnp.exp(-gate))) * up).astype(low)
            share(base + pn.mn, pn.gu, l, pn.ng, True)

        loop(0, pn.ng, gated)

        def out(j):
            l = j + pn.ng
            s = mod(l, DEPTH)
            ahead_m(i, l)
            wait(load_d(j, s))
            acc = jnp.dot(hid[...], wbuf[s, : pn.ff, :], preferred_element_type=f32)
            produce(acc, HALF + (i * NC + j) * 2, j)
            ticks(pn.m_dn(i, j), pn.m_dn(i, j + 1), True)

        loop(0, NC, out)

    def x_copy(i, j):
        n = T // XCUT
        at = pl.ds(pl.multiple_of(i * T + j * n, n), n)
        return pltpu.make_async_copy(x_ref.at[at, :], hbuf.at[at, :], x_sem.at[i, j])

    small = [pltpu.make_async_copy(a, b, c_sem.at[n])
             for n, (a, b) in enumerate([(ga_in, ga_ref), (rc_in, rc_ref), (rs_in, rs_ref), (gm_in, gm_ref)])]
    start(small[:1])
    for k in range(XCUT // 2):
        x_copy(0, k).start()
    start_a(jnp.int32(0))
    start(small[1:])
    for k in range(XCUT // 2, XCUT):
        x_copy(0, k).start()

    barrier = pltpu.get_barrier_semaphore()
    for to in (partner, pair):
        pl.semaphore_signal(barrier, inc=1, device_id={"tp": to}, device_id_type=MESH)

    @pl.when(is_mid)
    def _():
        pl.semaphore_signal(barrier, inc=1, device_id={"tp": across}, device_id_type=MESH)

    def greeted():
        @pl.when(is_mid)
        def _():
            pl.semaphore_wait(barrier, 3)

        @pl.when(is_end)
        def _():
            pl.semaphore_wait(barrier, 2)

    a_part(0, 0, False)
    a_part(1, 0, False)
    loop(1, pn.seqs, lambda i: a_part(2, i, i == pn.seqs - 1))
    loop(0, pn.seqs, m_part)
    flush(NU, 2 * JOIN)
    loop(0, PAIR, lambda s: d_copy(s).wait_send())
    last_ticks()


def check(pn):
    now, made, joined = 0, 0, 0

    def to(hi):
        nonlocal now
        assert hi >= now, (hi, now)
        now = hi
        assert now <= joined, (now, joined)

    def make(n):
        nonlocal made
        assert max(0, now - TO_MID) >= made + n - pn.slots, (now, made)
        made += n

    assert UP >= TO_END + 3 and pn.la % DEPTH == 0 and pn.lm % DEPTH == 0
    assert UP >= TO_END + 1 - (TO_SUM - TO_MID) and UP >= 2 * (TO_SUM - TO_MID) + 2 and PAIR >= 4 * JOIN + 4 and PAIR >= 8 * TWOS
    assert UP > 2 * (MID_PAIR - TO_SUM) + 1 and UP > 2 * (END_PAIR - TO_END) + 1
    for part in range(pn.seqs + 1):
        which = min(part, 2)
        before, counts, lead, _, n = pn.part(which, part - 1)
        assert now == before, (now, before)
        for count, steps in zip(counts, (PARTS, pn.nq, n // 128)):
            at = now
            for k in range(steps):
                to(at + count * (k + 1) // steps)
                joined = made
        at, inwo = now, counts[3]
        each = 4 if which == 2 else 2
        for j in range(pn.nc // 2):
            make(each)
            joined = made - TWOS * each if j >= TWOS else joined
            to(at + (inwo if j == pn.nc // 2 - 1 else (inwo * j + lead) // (pn.nc // 2)))
    for i in range(pn.seqs):
        assert now >= 2 * pn.nc * (i + 1) + END_PAIR, (i, now)
        base = pn.a_end + pn.km * i
        assert now == base
        for k in range(PARTS):
            to(base + pn.mn * (k + 1) // PARTS)
            joined = made
        base += pn.mn
        for k in range(pn.ng):
            to(base + pn.gu * (k + 1) // pn.ng)
        for j in range(pn.nc):
            make(2)
            joined = max(joined, made - 2 * JOIN) if j >= JOIN else joined
            to(base + pn.gu + (2 * j if i == pn.seqs - 1 else pn.dn * (j + 1) // pn.nc))
    assert made == pn.units and now == pn.done and now < pn.units and pn.a_end >= UP + END_PAIR and pn.units >= 2 * PAIR


def tables(rows):
    half = HEAD // 2
    angle = np.arange(rows, dtype=np.float32)[:, None] * np.float32(THETA) ** (-np.arange(half, dtype=np.float32) / np.float32(half))
    cos, sin = np.cos(angle), np.sin(angle)
    return np.concatenate([cos, cos], 1), np.concatenate([-sin, sin], 1)


def layer(x, gain_a, wq, wk, wv, wo, gain_m, w_gate, w_up, w_down):
    seqs, rows, d = x.shape
    pn = Plan(seqs, rows, d, wq.shape[1], w_gate.shape[1])
    check(pn)
    bf, f32, dma = jnp.bfloat16, jnp.float32, pltpu.SemaphoreType.DMA
    far = pl.BlockSpec(memory_space=pl.ANY)
    rc, rs = tables(rows)
    flops = 2 * seqs * rows * (d * (2 * pn.kq + 2 * HEAD) + 3 * d * pn.ff)
    y = pl.pallas_call(
        functools.partial(kernel, pn),
        out_shape=pltpu.VMEM((seqs * rows, d), bf),
        in_specs=[far] * 12,
        out_specs=pl.BlockSpec(memory_space=pltpu.VMEM),
        scratch_shapes=[
            pltpu.VMEM((rows, d), bf),
            pltpu.VMEM((DEPTH, d, COL), bf),
            pltpu.VMEM((rows, max(pn.ff, pn.kq)), bf),
            pltpu.VMEM((pn.heads, rows, HEAD), bf),
            pltpu.VMEM((rows, HEAD), bf),
            pltpu.VMEM((rows, HEAD), bf),
            pltpu.VMEM((pn.slots, pn.half, 128), f32),
            pltpu.VMEM((PAIR, pn.half, 128), bf),
            pltpu.VMEM((PAIR, pn.half, 128), bf),
            pltpu.VMEM((UP, pn.half, 128), bf),
            pltpu.VMEM((UP, pn.half, 128), bf),
            pltpu.VMEM((UP, pn.half, 128), bf),
            pltpu.VMEM((rows, COL), f32),
            pltpu.VMEM((d // 128, 128), bf),
            pltpu.VMEM((d // 128, 128), bf),
            pltpu.VMEM((rows, HEAD), f32),
            pltpu.VMEM((rows, HEAD), f32),
            dma((4,)),
            dma((seqs, XCUT)),
            dma((DEPTH, 2 * pn.per)),
            dma((PAIR,)),
            dma((PAIR,)),
            dma((UP,)),
            dma((UP,)),
            dma((UP,)),
            dma((UP,)),
            dma((UP,)),
            dma((UP,)),
            dma((UP,)),
        ],
        compiler_params=pltpu.CompilerParams(collective_id=0, has_side_effects=True, vmem_limit_bytes=43 * 2**20),
        cost_estimate=pl.CostEstimate(flops=flops, transcendentals=0, bytes_accessed=2 * (2 * x.size + wq.size + 3 * w_gate.size)),
    )(x.reshape(seqs * rows, d), gain_a.reshape(d // 128, 128), gain_m.reshape(d // 128, 128), rc, rs, wq, wk, wv, wo, w_gate, w_up, w_down)
    return put_out(y).reshape(x.shape)


def put_out(y):
    rows = y.shape[0] // OUT

    def body(y_ref, o_ref, sem):
        copies = [pltpu.make_async_copy(y_ref.at[k * rows : (k + 1) * rows], o_ref.at[k * rows : (k + 1) * rows], sem.at[k]) for k in range(OUT)]
        for x in copies:
            x.start()
        for x in copies:
            x.wait()

    return pl.pallas_call(
        body,
        out_shape=jax.ShapeDtypeStruct(y.shape, y.dtype),
        in_specs=[pl.BlockSpec(memory_space=pltpu.VMEM)],
        out_specs=pl.BlockSpec(memory_space=pl.ANY),
        scratch_shapes=[pltpu.SemaphoreType.DMA((OUT,))],
        compiler_params=pltpu.CompilerParams(vmem_limit_bytes=8 * 2**20),
    )(y)


def solution(mesh):
    tokens, whole, columns, rows_of = P("dp", None, None), P(None), P(None, "tp"), P("tp", None)
    return jax.shard_map(
        layer,
        mesh=mesh,
        in_specs=(tokens, whole, columns, columns, columns, rows_of, whole, columns, columns, rows_of),
        out_specs=tokens,
        check_vma=False,
    )
```
